16 devices in a mesh: dp: 2 (over z), tp: 8 (over y, x, core).
Axes of the slice: x: 2, y: 2, z: 2, core: 2. Of those that a mesh axis runs over, the one named last changes fastest.
Arguments:
- hidden_in: bfloat16 [64, 2048], P('dp'), parts along dimension 0
- k_cache: bfloat16 [64, 256, 16, 128], P('dp', None, 'tp'), parts along dimension 0
- v_cache: bfloat16 [64, 256, 16, 128], P('dp', None, 'tp'), parts along dimension 0
- seq_lens: int32 [64], P('dp'), parts along dimension 0
- chosen_experts: int32 [64, 6], P('dp'), parts along dimension 0
- g_attn: bfloat16 [2048], replicated
- w_q: bfloat16 [2048, 2048], P(None, 'tp')
- w_k: bfloat16 [2048, 2048], P(None, 'tp')
- w_v: bfloat16 [2048, 2048], P(None, 'tp')
- w_o: bfloat16 [2048, 2048], P('tp')
- g_moe: bfloat16 [2048], replicated
- w_router: bfloat16 [2048, 64], replicated
- w_gate: bfloat16 [64, 2048, 1408], P(None, None, 'tp')
- w_up: bfloat16 [64, 2048, 1408], P(None, None, 'tp')
- w_down: bfloat16 [64, 1408, 2048], P(None, 'tp')
Outputs:
- output 1: bfloat16 [64, 2048], P('dp'), parts along dimension 0
- output 2: bfloat16 [64, 256, 16, 128], P('dp', None, 'tp'), parts along dimension 0
- output 3: bfloat16 [64, 256, 16, 128], P('dp', None, 'tp'), parts along dimension 0
There are 2 independent parts. The reference program is written for one: setup_inputs(seed, part) draws one part's arguments, and reference() takes and returns one part's arrays. A program takes and returns all parts, laid end to end along the dimension named above; an argument that names none is the same for every part.
All inputs are finite; a program needn't handle non-finite values.
Results may differ from the reference program's by a relative error of at most 0.0145238.
Values are sent between devices in bfloat16 or wider.
A program may use at most 1 GiB of HBM per device.

```python
import math
import jax
import jax.numpy as jnp
from jax import lax

BATCH_SEQS = 32
CACHE_LEN = 256
D_MODEL = 2048
Q_HEADS = 16
KV_HEADS = 16
HEAD_DIM = 128
FFN_DIM = 1408
EXPERTS = 64
TOP_K = 6


def draw_layout(len_key, pick_key):
    seq_lens = jax.random.randint(len_key, (BATCH_SEQS,), 1, CACHE_LEN, dtype=jnp.int32)
    seq_lens = seq_lens.at[0].set(CACHE_LEN - 1)
    expert_ids = jnp.arange(EXPERTS, dtype=jnp.int32)
    hot_bonus = jnp.where(expert_ids < max(1, EXPERTS // 8), 2 * EXPERTS, 0)
    end_bonus = jnp.where((expert_ids == 0) | (expert_ids == EXPERTS - 1), 16 * EXPERTS, 0)
    first_row = (jnp.arange(BATCH_SEQS) == 0)[:, None]
    scores = jax.random.randint(pick_key, (BATCH_SEQS, EXPERTS), 0, 4 * EXPERTS, dtype=jnp.int32)
    scores = scores + hot_bonus[None, :] + jnp.where(first_row, end_bonus[None, :], 0)
    _, chosen_ids = lax.top_k(scores * EXPERTS + expert_ids[None, :], TOP_K)
    return seq_lens, chosen_ids.astype(jnp.int32)


def normal_weight(rng_key, out_shape, fan_in, factor):
    return (factor * fan_in ** -0.5 * jax.random.normal(rng_key, out_shape, jnp.float32)).astype(jnp.bfloat16)


def setup_inputs(seed: int = 0, part: int = 0) -> dict:
    part_keys = jax.random.split(jax.random.fold_in(jax.random.key(seed), part), 5)
    shared = jax.random.split(jax.random.key(seed + 1), 12)
    q_width = Q_HEADS * HEAD_DIM
    kv_width = KV_HEADS * HEAD_DIM
    key_scale = math.sqrt(0.75 * math.log(CACHE_LEN))
    cache_shape = (BATCH_SEQS, CACHE_LEN, KV_HEADS, HEAD_DIM)
    seq_lens, chosen_experts = draw_layout(part_keys[3], part_keys[4])
    return {
        "hidden_in": jax.random.normal(part_keys[0], (BATCH_SEQS, D_MODEL), jnp.float32).astype(jnp.bfloat16),
        "k_cache": (key_scale * jax.random.normal(part_keys[1], cache_shape, jnp.float32)).astype(jnp.bfloat16),
        "v_cache": jax.random.normal(part_keys[2], cache_shape, jnp.float32).astype(jnp.bfloat16),
        "seq_lens": seq_lens,
        "chosen_experts": chosen_experts,
        "g_attn": jax.random.uniform(shared[0], (D_MODEL,), jnp.float32, 0.5, 1.5).astype(jnp.bfloat16),
        "w_q": normal_weight(shared[1], (D_MODEL, q_width), D_MODEL, 1.0),
        "w_k": normal_weight(shared[2], (D_MODEL, kv_width), D_MODEL, 1.0),
        "w_v": normal_weight(shared[3], (D_MODEL, kv_width), D_MODEL, 1.0),
        "w_o": normal_weight(shared[4], (q_width, D_MODEL), q_width, 2.0),
        "g_moe": jax.random.uniform(shared[5], (D_MODEL,), jnp.float32, 0.5, 1.5).astype(jnp.bfloat16),
        "w_router": normal_weight(shared[6], (D_MODEL, EXPERTS), D_MODEL, 1.0),
        "w_gate": normal_weight(shared[7], (EXPERTS, D_MODEL, FFN_DIM), D_MODEL, 1.0),
        "w_up": normal_weight(shared[8], (EXPERTS, D_MODEL, FFN_DIM), D_MODEL, 1.0),
        "w_down": normal_weight(shared[9], (EXPERTS, FFN_DIM, D_MODEL), FFN_DIM, 2.0 * math.sqrt(TOP_K)),
    }


def rms_norm(vector, gain_w):
    vector32 = vector.astype(jnp.float32)
    norm_scale = lax.rsqrt(jnp.mean(vector32 * vector32, axis=-1, keepdims=True) + 1e-5)
    return (vector32 * norm_scale * gain_w.astype(jnp.float32)).astype(jnp.bfloat16)


def rope_rotate(vector, cos_t, sin_t):
    half_dim = vector.shape[-1] // 2
    lead_half = vector[..., :half_dim]
    tail_half = vector[..., half_dim:]
    return jnp.concatenate([lead_half * cos_t - tail_half * sin_t, tail_half * cos_t + lead_half * sin_t], axis=-1)


def attend_one(operands):
    q_seq, k_seq, v_seq, seq_len = operands
    scores = jnp.einsum("kgd,skd->kgs", q_seq.astype(jnp.float32), k_seq.astype(jnp.float32)) * HEAD_DIM ** -0.5
    in_range = (jnp.arange(CACHE_LEN) <= seq_len)[None, None, :]
    attn_weights = jax.nn.softmax(jnp.where(in_range, scores, -1e30), axis=-1).astype(jnp.bfloat16)
    return jnp.einsum("kgs,skd->kgd", attn_weights.astype(jnp.float32), v_seq.astype(jnp.float32)).astype(jnp.bfloat16)


def reference(hidden_in, k_cache, v_cache, seq_lens, chosen_experts, g_attn, w_q, w_k, w_v, w_o, g_moe, w_router, w_gate, w_up, w_down):
    q_group = Q_HEADS // KV_HEADS
    h_attn = rms_norm(hidden_in, g_attn)
    q_lin = jnp.dot(h_attn, w_q, preferred_element_type=jnp.float32).reshape(BATCH_SEQS, KV_HEADS, q_group, HEAD_DIM)
    k_lin = jnp.dot(h_attn, w_k, preferred_element_type=jnp.float32).reshape(BATCH_SEQS, KV_HEADS, HEAD_DIM)
    v_new = jnp.dot(h_attn, w_v, preferred_element_type=jnp.float32).reshape(BATCH_SEQS, KV_HEADS, HEAD_DIM).astype(jnp.bfloat16)
    inv_freq = 1000000.0 ** (-jnp.arange(0, HEAD_DIM, 2, dtype=jnp.float32) / HEAD_DIM)
    angles = seq_lens.astype(jnp.float32)[:, None] * inv_freq[None, :]
    cos_t = jnp.cos(angles)[:, None, :]
    sin_t = jnp.sin(angles)[:, None, :]
    q_rot = rope_rotate(q_lin, cos_t[:, :, None, :], sin_t[:, :, None, :]).astype(jnp.bfloat16)
    k_new = rope_rotate(k_lin, cos_t, sin_t).astype(jnp.bfloat16)
    new_slot = (jnp.arange(CACHE_LEN)[None, :] == seq_lens[:, None])[:, :, None, None]
    k_next = jnp.where(new_slot, k_new[:, None, :, :], k_cache)
    v_next = jnp.where(new_slot, v_new[:, None, :, :], v_cache)
    heads_out = lax.map(attend_one, (q_rot, k_next, v_next, seq_lens))
    attn_sum = jnp.dot(heads_out.reshape(BATCH_SEQS, Q_HEADS * HEAD_DIM), w_o, preferred_element_type=jnp.float32)
    hidden_mid = (hidden_in.astype(jnp.float32) + attn_sum).astype(jnp.bfloat16)
    h_moe = rms_norm(hidden_mid, g_moe)
    logits = jnp.dot(h_moe, w_router, preferred_element_type=jnp.float32)
    pick_mask = (chosen_experts[:, :, None] == jnp.arange(EXPERTS)[None, None, :]).astype(jnp.float32)
    gate_probs = jax.nn.softmax(jnp.sum(pick_mask * logits[:, None, :], axis=-1), axis=-1)
    gate_mat = jnp.sum(gate_probs[:, :, None] * pick_mask, axis=1)

    def expert_step(running, operands):
        gate_w, up_w, down_w, gate_col = operands
        up_gate = jnp.dot(h_moe, gate_w, preferred_element_type=jnp.float32)
        up_lin = jnp.dot(h_moe, up_w, preferred_element_type=jnp.float32)
        inner_act = (gate_col[:, None] * jax.nn.silu(up_gate) * up_lin).astype(jnp.bfloat16)
        return running + jnp.dot(inner_act, down_w, preferred_element_type=jnp.float32), None

    moe_sum, _ = lax.scan(expert_step, jnp.zeros((BATCH_SEQS, D_MODEL), jnp.float32), (w_gate, w_up, w_down, gate_mat.T))
    hidden_out = (hidden_mid.astype(jnp.float32) + moe_sum).astype(jnp.bfloat16)
    return (hidden_out, k_next, v_next)
```

```python
import functools

import jax
import jax.numpy as jnp
import numpy as np
from jax import lax
from jax.experimental import pallas as pl
from jax.experimental.pallas import tpu as pltpu
from jax.sharding import PartitionSpec as P

EPSILON = 1e-5
ROPE_THETA = 1000000.0
MASK_FILL = -1e30
F32 = jnp.float32
BF16 = jnp.bfloat16
ANY = pl.BlockSpec(memory_space=pltpu.HBM)
VMEM = pl.BlockSpec(memory_space=pltpu.VMEM)
SMEM = pl.BlockSpec(memory_space=pltpu.SMEM)
NT = (((1,), (1,)), ((), ()))

GROUP = 8
RING = 8


def norm_rows(x, gain):
    x32 = x.astype(F32)
    scale = lax.rsqrt(jnp.mean(x32 * x32, axis=-1, keepdims=True) + EPSILON)
    gain32 = gain.astype(F32)
    gain_row = jnp.concatenate([gain32[i:i + 1, :] for i in range(gain.shape[0])], axis=1)
    return (x32 * scale * gain_row).astype(BF16)


def attention_kernel(x_ref, lens_ref, chosen_ref, gain_ref, freq_ref, wq_hbm, wk_hbm, wv_hbm, wo_hbm, k_hbm, v_hbm,
                     part_ref, list_ref, ko_hbm, vo_hbm,
                     wq, wk, wv, wo, kbuf, vbuf, qs, ks, vs, os, wsem, ksem, vsem, kosem, vosem):
    rows, width = x_ref.shape
    slots2, dim = kbuf.shape[1], kbuf.shape[2]
    steps = rows // GROUP

    def load(hbm, buf, sem):
        return pltpu.make_async_copy(hbm, buf, sem)

    def part(hbm, buf, sem, c):
        block = pl.ds(c * GROUP, GROUP)
        return pltpu.make_async_copy(hbm.at[block], buf.at[block], sem.at[c])

    weights = [load(wq_hbm, wq, wsem.at[0]), load(wk_hbm, wk, wsem.at[1]), load(wv_hbm, wv, wsem.at[2]), load(wo_hbm, wo, wsem.at[3])]
    for copy in weights[:3]:
        copy.start()
    for c in range(steps):
        part(k_hbm, kbuf, ksem, c).start()
        part(v_hbm, vbuf, vsem, c).start()
    weights[3].start()

    experts = 64
    sub = lax.broadcasted_iota(jnp.int32, (experts, rows), 0)
    hit = chosen_ref[0:1, :] == sub
    for k in range(1, chosen_ref.shape[0]):
        hit = hit | (chosen_ref[k:k + 1, :] == sub)
    used_col = jnp.max(hit.astype(F32), axis=1, keepdims=True)
    si = lax.broadcasted_iota(jnp.int32, (experts, 128), 0)
    li = lax.broadcasted_iota(jnp.int32, (experts, 128), 1)
    used_row = jnp.sum(jnp.where(si == li, used_col, 0.0), axis=0, keepdims=True)
    rank_col = jnp.sum(jnp.where(li < si, used_row, 0.0), axis=1, keepdims=True)
    pick = (rank_col == li.astype(F32)) & (used_col > 0.0)
    ids = jnp.sum(jnp.where(pick, si.astype(F32), 0.0), axis=0, keepdims=True)
    total = jnp.sum(used_row, axis=1, keepdims=True)
    lane1 = lax.broadcasted_iota(jnp.int32, (1, 128), 1)
    list_ref[...] = jnp.where(lane1 == 127, total, ids).astype(jnp.int32)

    h = norm_rows(x_ref[...], gain_ref[...])

    row_id = lax.broadcasted_iota(jnp.int32, (rows, dim), 0)
    pos = jnp.zeros((rows, dim), F32)
    for b in range(rows):
        pos = jnp.where(row_id == b, lens_ref[b].astype(F32), pos)
    angle = pos * freq_ref[...]
    cos_t = jnp.cos(angle)
    lane = lax.broadcasted_iota(jnp.int32, (rows, dim), 1)
    sin_t = jnp.where(lane < dim // 2, -jnp.sin(angle), jnp.sin(angle))

    def rope(y):
        return y * cos_t + pltpu.roll(y, dim // 2, 1) * sin_t

    def project(copy, w):
        copy.wait()
        return jnp.dot(h, w[...], preferred_element_type=F32)

    q = project(weights[0], wq)
    k = project(weights[1], wk)
    v = project(weights[2], wv)
    for j in range(2):
        cols = slice(j * dim, (j + 1) * dim)
        qs[:, cols] = rope(q[:, cols]).astype(BF16).astype(F32)
        ks[:, cols] = rope(k[:, cols]).astype(BF16).astype(F32)
        vs[:, cols] = v[:, cols].astype(BF16).astype(F32)

    r16 = lax.broadcasted_iota(jnp.int32, (16, dim), 0)
    srow = lax.broadcasted_iota(jnp.int32, (16, slots2), 0)
    scol = lax.broadcasted_iota(jnp.int32, (16, slots2), 1)
    same_head = (srow % 2) == (scol % 2)
    slot = scol // 2

    def put_row(buf, new, b, p):
        tile = pl.ds(pl.multiple_of((p // 8) * 16, 16), 16)
        old = buf[b, tile, :].astype(F32)
        head = jnp.where(r16 % 2 == 0, new[pl.ds(b, 1), 0:dim], new[pl.ds(b, 1), dim:2 * dim])
        buf[b, tile, :] = jnp.where(r16 // 2 == p % 8, head, old).astype(BF16)

    for c in range(steps):
        part(k_hbm, kbuf, ksem, c).wait()
        part(v_hbm, vbuf, vsem, c).wait()
        qblocks = []
        limit = jnp.zeros((16, slots2), jnp.int32)
        for j in range(GROUP):
            b = c * GROUP + j
            p = lens_ref[b]
            put_row(kbuf, ks, b, p)
            put_row(vbuf, vs, b, p)
            limit = jnp.where(srow // 2 == j, p, limit)
            qblocks.append(jnp.where(r16 == 2 * j, qs[b:b + 1, 0:dim], jnp.where(r16 == 2 * j + 1, qs[b:b + 1, dim:2 * dim], 0.0)))
        score = jnp.zeros((16, slots2), F32)
        for j in range(0, GROUP, 2):
            b = c * GROUP + j
            lhs = jnp.concatenate([qblocks[j], qblocks[j + 1]], axis=1).astype(BF16)
            rhs = jnp.concatenate([kbuf[b], kbuf[b + 1]], axis=1)
            score = score + lax.dot_general(lhs, rhs, NT, preferred_element_type=F32)
        score = score * (dim ** -0.5)
        valid = same_head & (slot <= limit)
        score = jnp.where(valid, score, MASK_FILL)
        top = jnp.max(score, axis=1, keepdims=True)
        e = jnp.where(valid, jnp.exp(score - top), 0.0)
        w = (e / jnp.sum(e, axis=1, keepdims=True)).astype(BF16)
        out = jnp.zeros((16, dim), F32)
        for j in range(0, GROUP, 2):
            b = c * GROUP + j
            rhs = jnp.concatenate([vbuf[b], vbuf[b + 1]], axis=1)
            both = jnp.dot(w, rhs, preferred_element_type=F32)
            out = jnp.where(r16 // 2 == j, both[:, 0:dim], out)
            out = jnp.where(r16 // 2 == j + 1, both[:, dim:2 * dim], out)
        os[c * 16:(c + 1) * 16, :] = out
        part(kbuf, ko_hbm, kosem, c).start()
        part(vbuf, vo_hbm, vosem, c).start()

    heads = jnp.concatenate([os[pl.ds(0, rows, stride=2), :], os[pl.ds(1, rows, stride=2), :]], axis=1).astype(BF16)
    weights[3].wait()
    for j in range(0, width, 256):
        part_ref[:, j:j + 256] = jnp.dot(heads, wo[:, j:j + 256], preferred_element_type=F32)
    for c in range(steps):
        part(kbuf, ko_hbm, kosem, c).wait()
        part(vbuf, vo_hbm, vosem, c).wait()


def attention(x, lens, chosen_t, gain, freq, wq, wk, wv, wo, k_cache, v_cache):
    rows, width = x.shape
    steps = rows // GROUP
    return pl.pallas_call(
        attention_kernel,
        name="attention",
        out_shape=(
            jax.ShapeDtypeStruct((rows, width), F32),
            jax.ShapeDtypeStruct((1, 128), jnp.int32),
            jax.ShapeDtypeStruct(k_cache.shape, BF16),
            jax.ShapeDtypeStruct(v_cache.shape, BF16),
        ),
        in_specs=[VMEM, SMEM, VMEM, VMEM, VMEM] + [ANY] * 6,
        out_specs=(VMEM, VMEM, ANY, ANY),
        scratch_shapes=[
            pltpu.VMEM(wq.shape, BF16), pltpu.VMEM(wk.shape, BF16), pltpu.VMEM(wv.shape, BF16), pltpu.VMEM(wo.shape, BF16),
            pltpu.VMEM(k_cache.shape, BF16), pltpu.VMEM(v_cache.shape, BF16),
            pltpu.VMEM((rows, 256), F32), pltpu.VMEM((rows, 256), F32), pltpu.VMEM((rows, 256), F32),
            pltpu.VMEM((2 * rows, 128), F32),
            pltpu.SemaphoreType.DMA((4,)),
            pltpu.SemaphoreType.DMA((steps,)), pltpu.SemaphoreType.DMA((steps,)),
            pltpu.SemaphoreType.DMA((steps,)), pltpu.SemaphoreType.DMA((steps,)),
        ],
        compiler_params=pltpu.CompilerParams(vmem_limit_bytes=62 * 1024 * 1024),
    )(x, lens, chosen_t, gain, freq, wq, wk, wv, wo, k_cache, v_cache)


def sum_kernel(n, part_ref, base_ref, out_ref, inbox, piece, send1, recv1, send2, recv2):
    me = lax.axis_index("tp")
    cols = part_ref.shape[1] // n
    barrier = pltpu.get_barrier_semaphore()
    for d in range(1, n):
        pl.semaphore_signal(barrier, inc=1, device_id={"tp": lax.rem(me + d, n)}, device_id_type=pl.DeviceIdType.MESH)
    pl.semaphore_wait(barrier, n - 1)

    def columns(j):
        return pl.ds(pl.multiple_of(j * cols, cols), cols)

    first = []
    for d in range(1, n):
        to = lax.rem(me + d, n)
        copy = pltpu.make_async_remote_copy(
            src_ref=part_ref.at[:, columns(to)], dst_ref=inbox.at[d - 1],
            send_sem=send1.at[d - 1], recv_sem=recv1.at[d - 1],
            device_id={"tp": to}, device_id_type=pl.DeviceIdType.MESH)
        copy.start()
        first.append(copy)
    total = part_ref[:, columns(me)]
    for d in range(1, n):
        first[d - 1].wait_recv()
        total = total + inbox[d - 1]
    piece[...] = (base_ref[:, columns(me)].astype(F32) + total).astype(BF16)
    second = []
    for d in range(1, n):
        to = lax.rem(me + d, n)
        copy = pltpu.make_async_remote_copy(
            src_ref=piece, dst_ref=out_ref.at[:, columns(me)],
            send_sem=send2.at[d - 1], recv_sem=recv2.at[d - 1],
            device_id={"tp": to}, device_id_type=pl.DeviceIdType.MESH)
        copy.start()
        second.append(copy)
    out_ref[:, columns(me)] = piece[...]
    for d in range(1, n):
        first[d - 1].wait_send()
    for d in range(1, n):
        second[d - 1].wait()


def add_sum(part, base, n, collective_id):
    rows, width = base.shape
    return pl.pallas_call(
        functools.partial(sum_kernel, n),
        name="add_sum",
        out_shape=jax.ShapeDtypeStruct(base.shape, BF16),
        in_specs=[VMEM, VMEM],
        out_specs=VMEM,
        scratch_shapes=[
            pltpu.VMEM((n - 1, rows, width // n), F32), pltpu.VMEM((rows, width // n), BF16),
            pltpu.SemaphoreType.DMA((n - 1,)), pltpu.SemaphoreType.DMA((n - 1,)),
            pltpu.SemaphoreType.DMA((n - 1,)), pltpu.SemaphoreType.DMA((n - 1,)),
        ],
        compiler_params=pltpu.CompilerParams(collective_id=collective_id, has_side_effects=True, vmem_limit_bytes=8 * 1024 * 1024),
    )(part, base)


def experts_kernel(list_ref, x_ref, chosen_ref, gain_ref, wr_ref, gate_hbm, up_hbm, down_hbm, out_ref,
                   gates, h_ref, z_ref, ring_g, ring_u, ring_d, sem):
    rows, width = x_ref.shape
    count = list_ref[0, 127]

    def fetch(i, go):
        slot = lax.rem(i, RING)
        e = list_ref[0, jnp.minimum(i, count - 1)]
        for m, (hbm, ring) in enumerate(((gate_hbm, ring_g), (up_hbm, ring_u), (down_hbm, ring_d))):
            copy = pltpu.make_async_copy(hbm.at[e], ring.at[slot], sem.at[m, slot])
            if go:
                copy.start()
            else:
                copy.wait()

    for i in range(RING - 1):
        @pl.when(i < count)
        def _():
            fetch(i, True)

    h = norm_rows(x_ref[...], gain_ref[...])
    h_ref[...] = h
    logits = lax.dot_general(wr_ref[...], h, NT, preferred_element_type=F32)
    experts = logits.shape[0]
    sub = lax.broadcasted_iota(jnp.int32, (experts, rows), 0)
    hit = chosen_ref[0:1, :] == sub
    for k in range(1, chosen_ref.shape[0]):
        hit = hit | (chosen_ref[k:k + 1, :] == sub)
    top = jnp.max(jnp.where(hit, logits, MASK_FILL), axis=0, keepdims=True)
    e = jnp.where(hit, jnp.exp(jnp.where(hit, logits - top, 0.0)), 0.0)
    gates[...] = (e / jnp.sum(e, axis=0, keepdims=True)).T
    out_ref[...] = jnp.zeros_like(out_ref)
    lane = lax.broadcasted_iota(jnp.int32, (rows, experts), 1)

    def step(i, carry):
        @pl.when(i + RING - 1 < count)
        def _():
            fetch(i + RING - 1, True)

        fetch(i, False)
        slot = lax.rem(i, RING)
        e = list_ref[0, i]
        column = jnp.sum(jnp.where(lane == e, gates[...], 0.0), axis=1, keepdims=True)
        hh = h_ref[...]
        g = lax.dot_general(hh, ring_g[slot], NT, preferred_element_type=F32)
        u = lax.dot_general(hh, ring_u[slot], NT, preferred_element_type=F32)
        z = (column * jax.nn.silu(g) * u).astype(BF16)
        out_ref[...] += jnp.dot(z, ring_d[slot], preferred_element_type=F32)
        return carry

    lax.fori_loop(0, count, step, 0)


def experts_part(ids, x1, chosen_t, gain, wr_t, gate_t, up_t, down):
    rows, width = x1.shape
    n_experts, hidden = gate_t.shape[:2]
    return pl.pallas_call(
        experts_kernel,
        name="experts",
        out_shape=jax.ShapeDtypeStruct((rows, width), F32),
        in_specs=[SMEM, VMEM, VMEM, VMEM, VMEM, ANY, ANY, ANY],
        out_specs=VMEM,
        scratch_shapes=[
            pltpu.VMEM((rows, n_experts), F32), pltpu.VMEM((rows, width), BF16), pltpu.VMEM((rows, hidden), BF16),
            pltpu.VMEM((RING, hidden, width), BF16), pltpu.VMEM((RING, hidden, width), BF16), pltpu.VMEM((RING, hidden, width), BF16),
            pltpu.SemaphoreType.DMA((3, RING)),
        ],
        compiler_params=pltpu.CompilerParams(vmem_limit_bytes=40 * 1024 * 1024),
    )(ids, x1, chosen_t, gain, wr_t, gate_t, up_t, down)


def solution(mesh):
    n = mesh.shape["tp"]
    cache_spec = P("dp", None, "tp", None)
    in_specs = (P("dp", None), cache_spec, cache_spec, P("dp"), P("dp", None), P(None), P(None, "tp"), P(None, "tp"), P(None, "tp"), P("tp", None), P(None), P(None, None), P(None, None, "tp"), P(None, None, "tp"), P(None, "tp", None))
    out_specs = (P("dp", None), cache_spec, cache_spec)
    freq = (np.float32(ROPE_THETA) ** (-np.arange(0, 128, 2, dtype=np.float32) / np.float32(128))).astype(np.float32)
    freq = np.concatenate([freq, freq])[None, :]

    def layer_shard(hidden_in, k_cache, v_cache, seq_lens, chosen, g_attn, w_q, w_k, w_v, w_o, g_moe, w_router, w_gate, w_up, w_down):
        rows, slots, heads, dim = k_cache.shape
        width = hidden_in.shape[1]
        chosen_t = chosen.T
        flat = (rows, slots * heads, dim)
        part, ids, k_next, v_next = attention(
            hidden_in, seq_lens, chosen_t, g_attn.reshape(width // 128, 128), jnp.asarray(freq), w_q, w_k, w_v, w_o,
            k_cache.reshape(flat), v_cache.reshape(flat))
        x1 = add_sum(part, hidden_in, n, 1)
        moe = experts_part(ids, x1, chosen_t, g_moe.reshape(width // 128, 128), w_router.T,
                           jnp.swapaxes(w_gate, 1, 2), jnp.swapaxes(w_up, 1, 2), w_down)
        out = add_sum(moe, x1, n, 2)
        return out, k_next.reshape(k_cache.shape), v_next.reshape(v_cache.shape)

    return jax.shard_map(layer_shard, mesh=mesh, in_specs=in_specs, out_specs=out_specs, check_vma=False)
```

```python
import functools

import jax
import jax.numpy as jnp
import numpy as np
from jax import lax
from jax.experimental import pallas as pl
from jax.experimental.pallas import tpu as pltpu
from jax.sharding import PartitionSpec as P

EPSILON = 1e-5
ROPE_THETA = 1000000.0
MASK_FILL = -1e30
F32 = jnp.float32
BF16 = jnp.bfloat16
ANY = pl.BlockSpec(memory_space=pltpu.HBM)
VMEM = pl.BlockSpec(memory_space=pltpu.VMEM)
SMEM = pl.BlockSpec(memory_space=pltpu.SMEM)
NT = (((1,), (1,)), ((), ()))

GROUP = 8
RING = 8
HELD = 12


def norm_rows(x, gain):
    x32 = x.astype(F32)
    scale = lax.rsqrt(jnp.mean(x32 * x32, axis=-1, keepdims=True) + EPSILON)
    gain32 = gain.astype(F32)
    gain_row = jnp.concatenate([gain32[i:i + 1, :] for i in range(gain.shape[0])], axis=1)
    return (x32 * scale * gain_row).astype(BF16)


def attention_kernel(x_ref, lens_ref, chosen_ref, gain_ref, freq_ref, wq_hbm, wk_hbm, wv_hbm, wo_hbm, k_hbm, v_hbm,
                     part_ref, list_ref, ko_hbm, vo_hbm,
                     wq, wk, wv, wo, kbuf, vbuf, qs, ks, vs, os, wsem, ksem, vsem, kosem, vosem):
    rows, width = x_ref.shape
    slots2, dim = kbuf.shape[1], kbuf.shape[2]
    steps = rows // GROUP

    def load(hbm, buf, sem):
        return pltpu.make_async_copy(hbm, buf, sem)

    def part(hbm, buf, sem, c):
        block = pl.ds(c * GROUP, GROUP)
        return pltpu.make_async_copy(hbm.at[block], buf.at[block], sem.at[c])

    weights = [load(wq_hbm, wq, wsem.at[0]), load(wk_hbm, wk, wsem.at[1]), load(wv_hbm, wv, wsem.at[2]), load(wo_hbm, wo, wsem.at[3])]
    for copy in weights[:3]:
        copy.start()
    for c in range(steps):
        part(k_hbm, kbuf, ksem, c).start()
        part(v_hbm, vbuf, vsem, c).start()
    weights[3].start()

    experts = 64
    sub = lax.broadcasted_iota(jnp.int32, (experts, rows), 0)
    hit = chosen_ref[0:1, :] == sub
    for k in range(1, chosen_ref.shape[0]):
        hit = hit | (chosen_ref[k:k + 1, :] == sub)
    used_col = jnp.max(hit.astype(F32), axis=1, keepdims=True)
    si = lax.broadcasted_iota(jnp.int32, (experts, 128), 0)
    li = lax.broadcasted_iota(jnp.int32, (experts, 128), 1)
    used_row = jnp.sum(jnp.where(si == li, used_col, 0.0), axis=0, keepdims=True)
    rank_col = jnp.sum(jnp.where(li < si, used_row, 0.0), axis=1, keepdims=True)
    pick = (rank_col == li.astype(F32)) & (used_col > 0.0)
    ids = jnp.sum(jnp.where(pick, si.astype(F32), 0.0), axis=0, keepdims=True)
    total = jnp.sum(used_row, axis=1, keepdims=True)
    lane1 = lax.broadcasted_iota(jnp.int32, (1, 128), 1)
    held = jnp.sum(jnp.where(lane1 < HELD, used_row, 0.0), axis=1, keepdims=True)
    list_ref[...] = jnp.where(lane1 == 127, total, jnp.where(lane1 == 126, held, ids)).astype(jnp.int32)

    h = norm_rows(x_ref[...], gain_ref[...])

    row_id = lax.broadcasted_iota(jnp.int32, (rows, dim), 0)
    pos = jnp.zeros((rows, dim), F32)
    for b in range(rows):
        pos = jnp.where(row_id == b, lens_ref[b].astype(F32), pos)
    angle = pos * freq_ref[...]
    cos_t = jnp.cos(angle)
    lane = lax.broadcasted_iota(jnp.int32, (rows, dim), 1)
    sin_t = jnp.where(lane < dim // 2, -jnp.sin(angle), jnp.sin(angle))

    def rope(y):
        return y * cos_t + pltpu.roll(y, dim // 2, 1) * sin_t

    def project(copy, w):
        copy.wait()
        return jnp.dot(h, w[...], preferred_element_type=F32)

    q = project(weights[0], wq)
    k = project(weights[1], wk)
    v = project(weights[2], wv)
    for j in range(2):
        cols = slice(j * dim, (j + 1) * dim)
        qs[:, cols] = rope(q[:, cols]).astype(BF16).astype(F32)
        ks[:, cols] = rope(k[:, cols]).astype(BF16).astype(F32)
        vs[:, cols] = v[:, cols].astype(BF16).astype(F32)

    r16 = lax.broadcasted_iota(jnp.int32, (16, dim), 0)
    srow = lax.broadcasted_iota(jnp.int32, (16, slots2), 0)
    scol = lax.broadcasted_iota(jnp.int32, (16, slots2), 1)
    same_head = (srow % 2) == (scol % 2)
    slot = scol // 2

    def put_row(buf, new, b, p):
        tile = pl.ds(pl.multiple_of((p // 8) * 16, 16), 16)
        old = buf[b, tile, :].astype(F32)
        head = jnp.where(r16 % 2 == 0, new[pl.ds(b, 1), 0:dim], new[pl.ds(b, 1), dim:2 * dim])
        buf[b, tile, :] = jnp.where(r16 // 2 == p % 8, head, old).astype(BF16)

    for c in range(steps):
        part(k_hbm, kbuf, ksem, c).wait()
        part(v_hbm, vbuf, vsem, c).wait()
        qblocks = []
        limit = jnp.zeros((16, slots2), jnp.int32)
        for j in range(GROUP):
            b = c * GROUP + j
            p = lens_ref[b]
            put_row(kbuf, ks, b, p)
            put_row(vbuf, vs, b, p)
            limit = jnp.where(srow // 2 == j, p, limit)
            qblocks.append(jnp.where(r16 == 2 * j, qs[b:b + 1, 0:dim], jnp.where(r16 == 2 * j + 1, qs[b:b + 1, dim:2 * dim], 0.0)))
        score = jnp.zeros((16, slots2), F32)
        for j in range(0, GROUP, 2):
            b = c * GROUP + j
            lhs = jnp.concatenate([qblocks[j], qblocks[j + 1]], axis=1).astype(BF16)
            rhs = jnp.concatenate([kbuf[b], kbuf[b + 1]], axis=1)
            score = score + lax.dot_general(lhs, rhs, NT, preferred_element_type=F32)
        score = score * (dim ** -0.5)
        valid = same_head & (slot <= limit)
        score = jnp.where(valid, score, MASK_FILL)
        top = jnp.max(score, axis=1, keepdims=True)
        e = jnp.where(valid, jnp.exp(score - top), 0.0)
        w = (e / jnp.sum(e, axis=1, keepdims=True)).astype(BF16)
        out = jnp.zeros((16, dim), F32)
        for j in range(0, GROUP, 2):
            b = c * GROUP + j
            rhs = jnp.concatenate([vbuf[b], vbuf[b + 1]], axis=1)
            both = jnp.dot(w, rhs, preferred_element_type=F32)
            out = jnp.where(r16 // 2 == j, both[:, 0:dim], out)
            out = jnp.where(r16 // 2 == j + 1, both[:, dim:2 * dim], out)
        os[c * 16:(c + 1) * 16, :] = out
        part(kbuf, ko_hbm, kosem, c).start()
        part(vbuf, vo_hbm, vosem, c).start()

    heads = jnp.concatenate([os[pl.ds(0, rows, stride=2), :], os[pl.ds(1, rows, stride=2), :]], axis=1).astype(BF16)
    weights[3].wait()
    for j in range(0, width, 256):
        part_ref[:, j:j + 256] = jnp.dot(heads, wo[:, j:j + 256], preferred_element_type=F32)
    for c in range(steps):
        part(kbuf, ko_hbm, kosem, c).wait()
        part(vbuf, vo_hbm, vosem, c).wait()


def attention(x, lens, chosen_t, gain, freq, wq, wk, wv, wo, k_cache, v_cache):
    rows, width = x.shape
    steps = rows // GROUP
    return pl.pallas_call(
        attention_kernel,
        name="attention",
        out_shape=(
            jax.ShapeDtypeStruct((rows, width), F32),
            jax.ShapeDtypeStruct((1, 128), jnp.int32),
            jax.ShapeDtypeStruct(k_cache.shape, BF16),
            jax.ShapeDtypeStruct(v_cache.shape, BF16),
        ),
        in_specs=[VMEM, SMEM, VMEM, VMEM, VMEM] + [ANY] * 6,
        out_specs=(VMEM, VMEM, ANY, ANY),
        scratch_shapes=[
            pltpu.VMEM(wq.shape, BF16), pltpu.VMEM(wk.shape, BF16), pltpu.VMEM(wv.shape, BF16), pltpu.VMEM(wo.shape, BF16),
            pltpu.VMEM(k_cache.shape, BF16), pltpu.VMEM(v_cache.shape, BF16),
            pltpu.VMEM((rows, 256), F32), pltpu.VMEM((rows, 256), F32), pltpu.VMEM((rows, 256), F32),
            pltpu.VMEM((2 * rows, 128), F32),
            pltpu.SemaphoreType.DMA((4,)),
            pltpu.SemaphoreType.DMA((steps,)), pltpu.SemaphoreType.DMA((steps,)),
            pltpu.SemaphoreType.DMA((steps,)), pltpu.SemaphoreType.DMA((steps,)),
        ],
        compiler_params=pltpu.CompilerParams(vmem_limit_bytes=62 * 1024 * 1024),
    )(x, lens, chosen_t, gain, freq, wq, wk, wv, wo, k_cache, v_cache)


def sum_kernel(n, n_ahead, part_ref, base_ref, *refs):
    ahead_hbm, (out_ref, *ahead), (inbox, piece, send1, recv1, send2, recv2, *sems) = (
        refs[:n_ahead], refs[n_ahead:2 * n_ahead + 1], refs[2 * n_ahead + 1:])
    me = lax.axis_index("tp")
    loads = [pltpu.make_async_copy(src.at[pl.ds(e, 2)], dst.at[pl.ds(e, 2)], sems[0].at[m, e // 2])
             for e in range(0, HELD, 2) for m, (src, dst) in enumerate(zip(ahead_hbm, ahead))]
    for load in loads:
        load.start()
    cols = part_ref.shape[1] // n
    barrier = pltpu.get_barrier_semaphore()
    for d in range(1, n):
        pl.semaphore_signal(barrier, inc=1, device_id={"tp": lax.rem(me + d, n)}, device_id_type=pl.DeviceIdType.MESH)
    pl.semaphore_wait(barrier, n - 1)

    def columns(j):
        return pl.ds(pl.multiple_of(j * cols, cols), cols)

    first = []
    for d in range(1, n):
        to = lax.rem(me + d, n)
        copy = pltpu.make_async_remote_copy(
            src_ref=part_ref.at[:, columns(to)], dst_ref=inbox.at[d - 1],
            send_sem=send1.at[d - 1], recv_sem=recv1.at[d - 1],
            device_id={"tp": to}, device_id_type=pl.DeviceIdType.MESH)
        copy.start()
        first.append(copy)
    total = part_ref[:, columns(me)]
    for d in range(1, n):
        first[d - 1].wait_recv()
        total = total + inbox[d - 1]
    piece[...] = (base_ref[:, columns(me)].astype(F32) + total).astype(BF16)
    second = []
    for d in range(1, n):
        to = lax.rem(me + d, n)
        copy = pltpu.make_async_remote_copy(
            src_ref=piece, dst_ref=out_ref.at[:, columns(me)],
            send_sem=send2.at[d - 1], recv_sem=recv2.at[d - 1],
            device_id={"tp": to}, device_id_type=pl.DeviceIdType.MESH)
        copy.start()
        second.append(copy)
    out_ref[:, columns(me)] = piece[...]
    for d in range(1, n):
        first[d - 1].wait_send()
    for d in range(1, n):
        second[d - 1].wait()
    for load in loads:
        load.wait()


def add_sum(part, base, n, collective_id, ahead=()):
    rows, width = base.shape
    return pl.pallas_call(
        functools.partial(sum_kernel, n, len(ahead)),
        name="add_sum",
        out_shape=[jax.ShapeDtypeStruct(base.shape, BF16)] + [pltpu.VMEM((HELD, *a.shape[1:]), a.dtype) for a in ahead],
        in_specs=[VMEM, VMEM] + [ANY] * len(ahead),
        out_specs=[VMEM] * (1 + len(ahead)),
        scratch_shapes=[
            pltpu.VMEM((n - 1, rows, width // n), F32), pltpu.VMEM((rows, width // n), BF16),
            pltpu.SemaphoreType.DMA((n - 1,)), pltpu.SemaphoreType.DMA((n - 1,)),
            pltpu.SemaphoreType.DMA((n - 1,)), pltpu.SemaphoreType.DMA((n - 1,)),
        ] + ([pltpu.SemaphoreType.DMA((len(ahead), HELD // 2))] if ahead else []),
        compiler_params=pltpu.CompilerParams(collective_id=collective_id, has_side_effects=True, vmem_limit_bytes=8 * 1024 * 1024),
    )(part, base, *ahead)


def experts_kernel(list_ref, x_ref, chosen_ref, gain_ref, wr_ref, held_g, held_u, held_d, gate_hbm, up_hbm, down_hbm, out_ref,
                   gates, h_ref, g_ref, u_ref, ring_g, ring_u, ring_d, sem):
    rows, width = x_ref.shape
    held, count = list_ref[0, 126], list_ref[0, 127]
    rest = count - held

    def fetch(i, go):
        slot = lax.rem(i, RING)
        e = list_ref[0, held + i]
        for m, (hbm, ring) in enumerate(((gate_hbm, ring_g), (up_hbm, ring_u), (down_hbm, ring_d))):
            copy = pltpu.make_async_copy(hbm.at[e], ring.at[slot], sem.at[m, slot])
            if go:
                copy.start()
            else:
                copy.wait()

    for i in range(RING - 2):
        @pl.when(i < rest)
        def _():
            fetch(i, True)

    h = norm_rows(x_ref[...], gain_ref[...])
    h_ref[...] = h
    logits = lax.dot_general(wr_ref[...], h, NT, preferred_element_type=F32)
    experts = logits.shape[0]
    sub = lax.broadcasted_iota(jnp.int32, (experts, rows), 0)
    hit = chosen_ref[0:1, :] == sub
    for k in range(1, chosen_ref.shape[0]):
        hit = hit | (chosen_ref[k:k + 1, :] == sub)
    top = jnp.max(jnp.where(hit, logits, MASK_FILL), axis=0, keepdims=True)
    e = jnp.where(hit, jnp.exp(jnp.where(hit, logits - top, 0.0)), 0.0)
    gates[...] = (e / jnp.sum(e, axis=0, keepdims=True)).T
    out_ref[...] = jnp.zeros_like(out_ref)
    lane = lax.broadcasted_iota(jnp.int32, (rows, experts), 1)
    tile = 256

    def inner(e):
        column = jnp.sum(jnp.where(lane == e, gates[...], 0.0), axis=1, keepdims=True)
        return (column * jax.nn.silu(g_ref[...]) * u_ref[...]).astype(BF16)

    def wide(gate, up):
        g = u = None
        for t in range(0, width, tile):
            hk = h_ref[:, t:t + tile]
            gt = lax.dot_general(hk, gate(t), NT, preferred_element_type=F32)
            ut = lax.dot_general(up(t), hk, NT, preferred_element_type=F32)
            g, u = (gt, ut) if g is None else (g + gt, u + ut)
        return g, u.T

    def narrow(z, down):
        for t in range(0, width, tile):
            out_ref[:, t:t + tile] += jnp.dot(z, down(t), preferred_element_type=F32)

    def views(refs, index):
        return [lambda t, ref=ref: ref[index, :, t:t + tile] for ref in refs]

    def clear():
        g_ref[...] = jnp.zeros_like(g_ref)
        u_ref[...] = jnp.zeros_like(u_ref)

    def step_held(i, carry):
        before = list_ref[0, jnp.maximum(i - 1, 0)]
        z = inner(before)
        g, u = wide(*views((held_g, held_u), list_ref[0, i]))
        narrow(z, *views((held_d,), before))
        g_ref[...], u_ref[...] = g, u
        return carry

    def step_rest(i, carry):
        @pl.when(i + RING - 2 < rest)
        def _():
            fetch(i + RING - 2, True)

        @pl.when(i < rest)
        def _():
            fetch(i, False)

        z = inner(list_ref[0, jnp.maximum(held + i - 1, 0)])
        g, u = wide(*views((ring_g, ring_u), lax.rem(i, RING)))
        narrow(z, *views((ring_d,), lax.rem(i + RING - 1, RING)))
        g_ref[...], u_ref[...] = g, u
        return carry

    clear()

    @pl.when(held > 0)
    def _():
        lax.fori_loop(0, held, step_held, 0)
        before = list_ref[0, held - 1]
        narrow(inner(before), *views((held_d,), before))
        clear()

    @pl.when(rest > 0)
    def _():
        ring_d[RING - 1] = jnp.zeros(ring_d.shape[1:], BF16)
        lax.fori_loop(0, rest + 1, step_rest, 0)


def experts_part(ids, x1, chosen_t, gain, wr_t, held, gate_t, up_t, down):
    rows, width = x1.shape
    n_experts, hidden = gate_t.shape[:2]
    return pl.pallas_call(
        experts_kernel,
        name="experts",
        out_shape=jax.ShapeDtypeStruct((rows, width), F32),
        in_specs=[SMEM, VMEM, VMEM, VMEM, VMEM, VMEM, VMEM, VMEM, ANY, ANY, ANY],
        out_specs=VMEM,
        scratch_shapes=[
            pltpu.VMEM((rows, n_experts), F32), pltpu.VMEM((rows, width), BF16),
            pltpu.VMEM((rows, hidden), F32), pltpu.VMEM((rows, hidden), F32),
            pltpu.VMEM((RING, hidden, width), BF16), pltpu.VMEM((RING, hidden, width), BF16), pltpu.VMEM((RING, hidden, width), BF16),
            pltpu.SemaphoreType.DMA((3, RING)),
        ],
        compiler_params=pltpu.CompilerParams(vmem_limit_bytes=20 * 1024 * 1024),
    )(ids, x1, chosen_t, gain, wr_t, *held, gate_t, up_t, down)


def solution(mesh):
    n = mesh.shape["tp"]
    cache_spec = P("dp", None, "tp", None)
    in_specs = (P("dp", None), cache_spec, cache_spec, P("dp"), P("dp", None), P(None), P(None, "tp"), P(None, "tp"), P(None, "tp"), P("tp", None), P(None), P(None, None), P(None, None, "tp"), P(None, None, "tp"), P(None, "tp", None))
    out_specs = (P("dp", None), cache_spec, cache_spec)
    freq = (np.float32(ROPE_THETA) ** (-np.arange(0, 128, 2, dtype=np.float32) / np.float32(128))).astype(np.float32)
    freq = np.concatenate([freq, freq])[None, :]

    def layer_shard(hidden_in, k_cache, v_cache, seq_lens, chosen, g_attn, w_q, w_k, w_v, w_o, g_moe, w_router, w_gate, w_up, w_down):
        rows, slots, heads, dim = k_cache.shape
        width = hidden_in.shape[1]
        chosen_t = chosen.T
        flat = (rows, slots * heads, dim)
        part, ids, k_next, v_next = attention(
            hidden_in, seq_lens, chosen_t, g_attn.reshape(width // 128, 128), jnp.asarray(freq), w_q, w_k, w_v, w_o,
            k_cache.reshape(flat), v_cache.reshape(flat))
        experts = (jnp.swapaxes(w_gate, 1, 2), jnp.swapaxes(w_up, 1, 2), w_down)
        x1, *held = add_sum(part, hidden_in, n, 1, experts)
        moe = experts_part(ids, x1, chosen_t, g_moe.reshape(width // 128, 128), w_router.T, held, *experts)
        out, = add_sum(moe, x1, n, 2)
        return out, k_next.reshape(k_cache.shape), v_next.reshape(v_cache.shape)

    return jax.shard_map(layer_shard, mesh=mesh, in_specs=in_specs, out_specs=out_specs, check_vma=False)
```

```python
import functools

import jax
import jax.numpy as jnp
import numpy as np
from jax import lax
from jax.experimental import pallas as pl
from jax.experimental.pallas import tpu as pltpu
from jax.sharding import PartitionSpec as P

EPSILON = 1e-5
ROPE_THETA = 1000000.0
MASK_FILL = -1e30
F32 = jnp.float32
BF16 = jnp.bfloat16
ANY = pl.BlockSpec(memory_space=pltpu.HBM)
VMEM = pl.BlockSpec(memory_space=pltpu.VMEM)
SMEM = pl.BlockSpec(memory_space=pltpu.SMEM)
NT = (((1,), (1,)), ((), ()))


def in_hbm(*arrays):
    return [pltpu.with_memory_space_constraint(a, pltpu.HBM) for a in arrays]


GROUP = 8
RING = 5
HELD = 16


def norm_rows(x, gain):
    x32 = x.astype(F32)
    scale = lax.rsqrt(jnp.mean(x32 * x32, axis=-1, keepdims=True) + EPSILON)
    gain32 = gain.astype(F32)
    gain_row = jnp.concatenate([gain32[i:i + 1, :] for i in range(gain.shape[0])], axis=1)
    return (x32 * scale * gain_row).astype(BF16)


def attention_kernel(x_hbm, lens_hbm, chosen_hbm, gain_hbm, freq_hbm, wq_hbm, wk_hbm, wv_hbm, k_hbm, v_hbm,
                     heads_ref, list_ref, ko_hbm, vo_hbm,
                     x_ref, lens_ref, chosen_ref, gain_ref, freq_ref, wq, wk, wv, kbuf, vbuf, qs, ks, vs, os,
                     wsem, ksem, vsem, kosem, vosem):
    rows, width = x_ref.shape
    slots2, dim = kbuf.shape[1], kbuf.shape[2]
    steps = rows // GROUP

    def load(hbm, buf, sem):
        return pltpu.make_async_copy(hbm, buf, sem)

    def part(hbm, buf, sem, c):
        block = pl.ds(c * GROUP, GROUP)
        return pltpu.make_async_copy(hbm.at[block], buf.at[block], sem.at[c])

    pairs = ((x_hbm, x_ref), (gain_hbm, gain_ref), (lens_hbm, lens_ref), (freq_hbm, freq_ref), (chosen_hbm, chosen_ref),
             (wq_hbm, wq), (wk_hbm, wk), (wv_hbm, wv))
    loads = [load(hbm, buf, wsem.at[i]) for i, (hbm, buf) in enumerate(pairs)]
    weights = loads[5:]
    for copy in loads:
        copy.start()
    for c in range(steps):
        part(k_hbm, kbuf, ksem, c).start()
        part(v_hbm, vbuf, vsem, c).start()
    for copy in loads[:5]:
        copy.wait()

    experts = 64
    sub = lax.broadcasted_iota(jnp.int32, (experts, rows), 0)
    hit = chosen_ref[0:1, :] == sub
    for k in range(1, chosen_ref.shape[0]):
        hit = hit | (chosen_ref[k:k + 1, :] == sub)
    used_col = jnp.max(hit.astype(F32), axis=1, keepdims=True)
    si = lax.broadcasted_iota(jnp.int32, (experts, 128), 0)
    li = lax.broadcasted_iota(jnp.int32, (experts, 128), 1)
    used_row = jnp.sum(jnp.where(si == li, used_col, 0.0), axis=0, keepdims=True)
    rank_col = jnp.sum(jnp.where(li < si, used_row, 0.0), axis=1, keepdims=True)
    pick = (rank_col == li.astype(F32)) & (used_col > 0.0)
    ids = jnp.sum(jnp.where(pick, si.astype(F32), 0.0), axis=0, keepdims=True)
    total = jnp.sum(used_row, axis=1, keepdims=True)
    lane1 = lax.broadcasted_iota(jnp.int32, (1, 128), 1)
    held = jnp.sum(jnp.where(lane1 < HELD, used_row, 0.0), axis=1, keepdims=True)
    list_ref[...] = jnp.where(lane1 == 127, total, jnp.where(lane1 == 126, held, ids)).astype(jnp.int32)

    h = norm_rows(x_ref[...], gain_ref[...])

    row_id = lax.broadcasted_iota(jnp.int32, (rows, dim), 0)
    pos = jnp.zeros((rows, dim), F32)
    for b in range(rows):
        pos = jnp.where(row_id == b, lens_ref[b].astype(F32), pos)
    angle = pos * freq_ref[...]
    cos_t = jnp.cos(angle)
    lane = lax.broadcasted_iota(jnp.int32, (rows, dim), 1)
    sin_t = jnp.where(lane < dim // 2, -jnp.sin(angle), jnp.sin(angle))

    def rope(y):
        return y * cos_t + pltpu.roll(y, dim // 2, 1) * sin_t

    def project(copy, w):
        copy.wait()
        return jnp.dot(h, w[...], preferred_element_type=F32)

    q = project(weights[0], wq)
    k = project(weights[1], wk)
    v = project(weights[2], wv)
    for j in range(2):
        cols = slice(j * dim, (j + 1) * dim)
        qs[:, cols] = rope(q[:, cols]).astype(BF16).astype(F32)
        ks[:, cols] = rope(k[:, cols]).astype(BF16).astype(F32)
        vs[:, cols] = v[:, cols].astype(BF16).astype(F32)

    r16 = lax.broadcasted_iota(jnp.int32, (16, dim), 0)
    srow = lax.broadcasted_iota(jnp.int32, (16, slots2), 0)
    scol = lax.broadcasted_iota(jnp.int32, (16, slots2), 1)
    same_head = (srow % 2) == (scol % 2)
    slot = scol // 2

    def put_row(buf, new, b, p):
        tile = pl.ds(pl.multiple_of((p // 8) * 16, 16), 16)
        old = buf[b, tile, :].astype(F32)
        head = jnp.where(r16 % 2 == 0, new[pl.ds(b, 1), 0:dim], new[pl.ds(b, 1), dim:2 * dim])
        buf[b, tile, :] = jnp.where(r16 // 2 == p % 8, head, old).astype(BF16)

    for c in range(steps):
        part(k_hbm, kbuf, ksem, c).wait()
        part(v_hbm, vbuf, vsem, c).wait()
        qblocks = []
        limit = jnp.zeros((16, slots2), jnp.int32)
        for j in range(GROUP):
            b = c * GROUP + j
            p = lens_ref[b]
            put_row(kbuf, ks, b, p)
            put_row(vbuf, vs, b, p)
            limit = jnp.where(srow // 2 == j, p, limit)
            qblocks.append(jnp.where(r16 == 2 * j, qs[b:b + 1, 0:dim], jnp.where(r16 == 2 * j + 1, qs[b:b + 1, dim:2 * dim], 0.0)))
        score = jnp.zeros((16, slots2), F32)
        for j in range(0, GROUP, 2):
            b = c * GROUP + j
            lhs = jnp.concatenate([qblocks[j], qblocks[j + 1]], axis=1).astype(BF16)
            rhs = jnp.concatenate([kbuf[b], kbuf[b + 1]], axis=1)
            score = score + lax.dot_general(lhs, rhs, NT, preferred_element_type=F32)
        score = score * (dim ** -0.5)
        valid = same_head & (slot <= limit)
        score = jnp.where(valid, score, MASK_FILL)
        top = jnp.max(score, axis=1, keepdims=True)
        e = jnp.where(valid, jnp.exp(score - top), 0.0)
        w = (e / jnp.sum(e, axis=1, keepdims=True)).astype(BF16)
        out = jnp.zeros((16, dim), F32)
        for j in range(0, GROUP, 2):
            b = c * GROUP + j
            rhs = jnp.concatenate([vbuf[b], vbuf[b + 1]], axis=1)
            both = jnp.dot(w, rhs, preferred_element_type=F32)
            out = jnp.where(r16 // 2 == j, both[:, 0:dim], out)
            out = jnp.where(r16 // 2 == j + 1, both[:, dim:2 * dim], out)
        os[c * 16:(c + 1) * 16, :] = out
        part(kbuf, ko_hbm, kosem, c).start()
        part(vbuf, vo_hbm, vosem, c).start()

    heads_ref[...] = jnp.concatenate([os[pl.ds(0, rows, stride=2), :], os[pl.ds(1, rows, stride=2), :]], axis=1).astype(BF16)
    for c in range(steps):
        part(kbuf, ko_hbm, kosem, c).wait()
        part(vbuf, vo_hbm, vosem, c).wait()


def attention(x, lens, chosen_t, gain, freq, wq, wk, wv, k_cache, v_cache):
    rows, width = x.shape
    steps = rows // GROUP
    return pl.pallas_call(
        attention_kernel,
        name="attention",
        out_shape=(
            pltpu.VMEM((rows, 256), BF16),
            pltpu.VMEM((1, 128), jnp.int32),
            jax.ShapeDtypeStruct(k_cache.shape, BF16),
            jax.ShapeDtypeStruct(v_cache.shape, BF16),
        ),
        in_specs=[ANY] * 10,
        out_specs=(VMEM, VMEM, ANY, ANY),
        scratch_shapes=[
            pltpu.VMEM(x.shape, BF16), pltpu.SMEM(lens.shape, jnp.int32), pltpu.VMEM(chosen_t.shape, jnp.int32),
            pltpu.VMEM(gain.shape, BF16), pltpu.VMEM(freq.shape, F32),
            pltpu.VMEM(wq.shape, BF16), pltpu.VMEM(wk.shape, BF16), pltpu.VMEM(wv.shape, BF16),
            pltpu.VMEM(k_cache.shape, BF16), pltpu.VMEM(v_cache.shape, BF16),
            pltpu.VMEM((rows, 256), F32), pltpu.VMEM((rows, 256), F32), pltpu.VMEM((rows, 256), F32),
            pltpu.VMEM((2 * rows, 128), F32),
            pltpu.SemaphoreType.DMA((8,)),
            pltpu.SemaphoreType.DMA((steps,)), pltpu.SemaphoreType.DMA((steps,)),
            pltpu.SemaphoreType.DMA((steps,)), pltpu.SemaphoreType.DMA((steps,)),
        ],
        compiler_params=pltpu.CompilerParams(vmem_limit_bytes=16 * 1024 * 1024),
    )(*in_hbm(x, lens, chosen_t, gain, freq, wq, wk, wv, k_cache, v_cache))


ORDER = (6, 2, 4, 7, 3, 5, 1)


def sum_kernel(n_ahead, project, *refs):
    if project:
        heads_ref, wo_hbm, *refs = refs
    else:
        part_ref, *refs = refs
    base_ref, *refs = refs
    ahead_hbm, (out_ref, *ahead), (inbox, piece, sems, *refs) = refs[:n_ahead], refs[n_ahead:2 * n_ahead + 1], refs[2 * n_ahead + 1:]
    me = lax.axis_index("tp")
    core, xx, yy = lax.rem(me, 2), lax.rem(me // 2, 2), me // 4
    cols = base_ref.shape[1] // 8

    def peer(m):
        return (1 - yy if m & 4 else yy) * 4 + (1 - xx if m & 2 else xx) * 2 + (1 - core if m & 1 else core)

    def columns(j):
        return pl.ds(pl.multiple_of(j * cols, cols), cols)

    def send(src, dst, m, phase):
        return pltpu.make_async_remote_copy(
            src_ref=src, dst_ref=dst, send_sem=sems.at[phase, m], recv_sem=sems.at[phase + 1, m],
            device_id={"tp": peer(m)}, device_id_type=pl.DeviceIdType.MESH)

    barrier = pltpu.get_barrier_semaphore()
    for m in ORDER:
        pl.semaphore_signal(barrier, inc=1, device_id={"tp": peer(m)}, device_id_type=pl.DeviceIdType.MESH)
    loads = []
    if project:
        wo, part_ref, load_sems = refs
        load_wo = pltpu.make_async_copy(wo_hbm, wo, sems.at[0, 0])
        load_wo.start()
        loads = [pltpu.make_async_copy(src.at[pl.ds(e, 2)], dst.at[pl.ds(e, 2)], load_sems.at[m, e // 2])
                 for e in range(0, HELD, 2) for m, (src, dst) in enumerate(zip(ahead_hbm, ahead))]
        for load in loads:
            load.start()
        load_wo.wait()
        for j in range(0, base_ref.shape[1], cols):
            part_ref[:, j:j + cols] = jnp.dot(heads_ref[...], wo[:, j:j + cols], preferred_element_type=F32)
    pl.semaphore_wait(barrier, len(ORDER))

    first = {m: send(part_ref.at[:, columns(peer(m))], inbox.at[m - 1], m, 0) for m in ORDER}
    for m in ORDER:
        first[m].start()
    total = part_ref[:, columns(me)]
    for m in (1, 2, 4, 3, 5, 6, 7):
        first[m].wait_recv()
        total = total + inbox[m - 1]
    piece[...] = (base_ref[:, columns(me)].astype(F32) + total).astype(BF16)
    second = [send(piece, out_ref.at[:, columns(me)], m, 2) for m in ORDER]
    for copy in second:
        copy.start()
    out_ref[:, columns(me)] = piece[...]
    for m in ORDER:
        first[m].wait_send()
    for copy in second:
        copy.wait()
    for load in loads:
        load.wait()


def add_sum(partial, base, collective_id, ahead=()):
    rows, width = base.shape
    project = len(partial) == 2
    scratch = [pltpu.VMEM((7, rows, width // 8), F32), pltpu.VMEM((rows, width // 8), BF16), pltpu.SemaphoreType.DMA((4, 8))]
    if project:
        partial = (partial[0], *in_hbm(partial[1]))
        scratch += [pltpu.VMEM(partial[1].shape, BF16), pltpu.VMEM((rows, width), F32), pltpu.SemaphoreType.DMA((3, HELD // 2))]
    return pl.pallas_call(
        functools.partial(sum_kernel, len(ahead), project),
        name="add_sum",
        out_shape=[pltpu.VMEM(base.shape, BF16)] + [pltpu.VMEM((HELD, *a.shape[1:]), a.dtype) for a in ahead],
        in_specs=[VMEM] + [ANY] * (len(partial) - 1) + [VMEM] + [ANY] * len(ahead),
        out_specs=[VMEM] * (1 + len(ahead)),
        scratch_shapes=scratch,
        compiler_params=pltpu.CompilerParams(collective_id=collective_id, has_side_effects=True, vmem_limit_bytes=4 * 1024 * 1024),
    )(*partial, base, *in_hbm(*ahead))


def experts_kernel(list_ref, x_ref, chosen_ref, gain_ref, wr_ref, held_g, held_u, held_d, gate_hbm, up_hbm, down_hbm, out_ref,
                   gates, h_ref, g_ref, u_ref, ring_g, ring_u, ring_d, sem):
    rows, width = x_ref.shape
    held, count = list_ref[0, 126], list_ref[0, 127]
    rest = count - held

    def fetch(i, go):
        slot = lax.rem(i, RING)
        e = list_ref[0, held + i]
        for m, (hbm, ring) in enumerate(((gate_hbm, ring_g), (up_hbm, ring_u), (down_hbm, ring_d))):
            copy = pltpu.make_async_copy(hbm.at[e], ring.at[slot], sem.at[m, slot])
            if go:
                copy.start()
            else:
                copy.wait()

    for i in range(RING - 2):
        @pl.when(i < rest)
        def _():
            fetch(i, True)

    h = norm_rows(x_ref[...], gain_ref[...])
    h_ref[...] = h
    logits = lax.dot_general(wr_ref[...], h, NT, preferred_element_type=F32)
    experts = logits.shape[0]
    sub = lax.broadcasted_iota(jnp.int32, (experts, rows), 0)
    hit = chosen_ref[0:1, :] == sub
    for k in range(1, chosen_ref.shape[0]):
        hit = hit | (chosen_ref[k:k + 1, :] == sub)
    top = jnp.max(jnp.where(hit, logits, MASK_FILL), axis=0, keepdims=True)
    e = jnp.where(hit, jnp.exp(jnp.where(hit, logits - top, 0.0)), 0.0)
    gates[...] = (e / jnp.sum(e, axis=0, keepdims=True)).T
    out_ref[...] = jnp.zeros_like(out_ref)
    lane = lax.broadcasted_iota(jnp.int32, (rows, experts), 1)
    tile = 256

    def inner(e):
        column = jnp.sum(jnp.where(lane == e, gates[...], 0.0), axis=1, keepdims=True)
        return (column * jax.nn.silu(g_ref[...]) * u_ref[...]).astype(BF16)

    def wide(gate, up):
        g = u = None
        for t in range(0, width, tile):
            hk = h_ref[:, t:t + tile]
            gt = lax.dot_general(hk, gate(t), NT, preferred_element_type=F32)
            ut = lax.dot_general(up(t), hk, NT, preferred_element_type=F32)
            g, u = (gt, ut) if g is None else (g + gt, u + ut)
        return g, u.T

    def narrow(z, down):
        for t in range(0, width, tile):
            out_ref[:, t:t + tile] += jnp.dot(z, down(t), preferred_element_type=F32)

    def views(refs, index):
        return [lambda t, ref=ref: ref[index, :, t:t + tile] for ref in refs]

    def clear():
        g_ref[...] = jnp.zeros_like(g_ref)
        u_ref[...] = jnp.zeros_like(u_ref)

    def step_held(i, carry):
        before = list_ref[0, jnp.maximum(i - 1, 0)]
        z = inner(before)
        g, u = wide(*views((held_g, held_u), list_ref[0, i]))
        narrow(z, *views((held_d,), before))
        g_ref[...], u_ref[...] = g, u
        return carry

    def step_rest(i, carry):
        @pl.when(i + RING - 2 < rest)
        def _():
            fetch(i + RING - 2, True)

        @pl.when(i < rest)
        def _():
            fetch(i, False)

        z = inner(list_ref[0, jnp.maximum(held + i - 1, 0)])
        g, u = wide(*views((ring_g, ring_u), lax.rem(i, RING)))
        narrow(z, *views((ring_d,), lax.rem(i + RING - 1, RING)))
        g_ref[...], u_ref[...] = g, u
        return carry

    clear()

    @pl.when(held > 0)
    def _():
        lax.fori_loop(0, held, step_held, 0)
        before = list_ref[0, held - 1]
        narrow(inner(before), *views((held_d,), before))
        clear()

    @pl.when(rest > 0)
    def _():
        ring_d[RING - 1] = jnp.zeros(ring_d.shape[1:], BF16)
        lax.fori_loop(0, rest + 1, step_rest, 0)


def experts_part(ids, x1, chosen_t, gain, wr_t, held, gate_t, up_t, down):
    rows, width = x1.shape
    n_experts, hidden = gate_t.shape[:2]
    return pl.pallas_call(
        experts_kernel,
        name="experts",
        out_shape=pltpu.VMEM((rows, width), F32),
        in_specs=[SMEM, VMEM, VMEM, VMEM, VMEM, VMEM, VMEM, VMEM, ANY, ANY, ANY],
        out_specs=VMEM,
        scratch_shapes=[
            pltpu.VMEM((rows, n_experts), F32), pltpu.VMEM((rows, width), BF16),
            pltpu.VMEM((rows, hidden), F32), pltpu.VMEM((rows, hidden), F32),
            pltpu.VMEM((RING, hidden, width), BF16), pltpu.VMEM((RING, hidden, width), BF16), pltpu.VMEM((RING, hidden, width), BF16),
            pltpu.SemaphoreType.DMA((3, RING)),
        ],
        compiler_params=pltpu.CompilerParams(vmem_limit_bytes=12 * 1024 * 1024),
    )(ids, x1, chosen_t, gain, wr_t, *held, *in_hbm(gate_t, up_t, down))


def solution(mesh):
    cache_spec = P("dp", None, "tp", None)
    in_specs = (P("dp", None), cache_spec, cache_spec, P("dp"), P("dp", None), P(None), P(None, "tp"), P(None, "tp"), P(None, "tp"), P("tp", None), P(None), P(None, None), P(None, None, "tp"), P(None, None, "tp"), P(None, "tp", None))
    out_specs = (P("dp", None), cache_spec, cache_spec)
    freq = (np.float32(ROPE_THETA) ** (-np.arange(0, 128, 2, dtype=np.float32) / np.float32(128))).astype(np.float32)
    freq = np.concatenate([freq, freq])[None, :]

    def layer_shard(hidden_in, k_cache, v_cache, seq_lens, chosen, g_attn, w_q, w_k, w_v, w_o, g_moe, w_router, w_gate, w_up, w_down):
        rows, slots, kv_heads, dim = k_cache.shape
        width = hidden_in.shape[1]
        chosen_t = chosen.T
        flat = (rows, slots * kv_heads, dim)
        heads, ids, k_next, v_next = attention(
            hidden_in, seq_lens, chosen_t, g_attn.reshape(width // 128, 128), jnp.asarray(freq), w_q, w_k, w_v,
            k_cache.reshape(flat), v_cache.reshape(flat))
        experts = (jnp.swapaxes(w_gate, 1, 2), jnp.swapaxes(w_up, 1, 2), w_down)
        x1, *held = add_sum((heads, w_o), hidden_in, 1, experts)
        moe = experts_part(ids, x1, chosen_t, g_moe.reshape(width // 128, 128), w_router.T, held, *experts)
        out, = add_sum((moe,), x1, 2)
        return out, k_next.reshape(k_cache.shape), v_next.reshape(v_cache.shape)

    return jax.shard_map(layer_shard, mesh=mesh, in_specs=in_specs, out_specs=out_specs, check_vma=False)
```

```python
import functools

import jax
import jax.numpy as jnp
import numpy as np
from jax import lax
from jax.experimental import pallas as pl
from jax.experimental.pallas import tpu as pltpu
from jax.sharding import PartitionSpec as P

EPSILON = 1e-5
ROPE_THETA = 1000000.0
MASK_FILL = -1e30
F32 = jnp.float32
BF16 = jnp.bfloat16
ANY = pl.BlockSpec(memory_space=pltpu.HBM)
VMEM = pl.BlockSpec(memory_space=pltpu.VMEM)
SMEM = pl.BlockSpec(memory_space=pltpu.SMEM)
NT = (((1,), (1,)), ((), ()))


def in_hbm(*arrays):
    return [pltpu.with_memory_space_constraint(a, pltpu.HBM) for a in arrays]


GROUP = 8
RING = 5
HELD = 16


def norm_rows(x, gain):
    x32 = x.astype(F32)
    scale = lax.rsqrt(jnp.mean(x32 * x32, axis=-1, keepdims=True) + EPSILON)
    gain32 = gain.astype(F32)
    gain_row = jnp.concatenate([gain32[i:i + 1, :] for i in range(gain.shape[0])], axis=1)
    return (x32 * scale * gain_row).astype(BF16)


def attention_kernel(x_hbm, lens_hbm, chosen_hbm, gain_hbm, freq_hbm, wq_hbm, wk_hbm, wv_hbm, k_hbm, v_hbm,
                     heads_ref, list_ref, ko_hbm, vo_hbm,
                     x_ref, lens_ref, chosen_ref, gain_ref, freq_ref, wq, wk, wv, kbuf, vbuf, qs, ks, vs, os,
                     wsem, ksem, vsem, kosem, vosem):
    rows, width = x_ref.shape
    slots2, dim = kbuf.shape[1], kbuf.shape[2]
    steps = rows // GROUP

    def load(hbm, buf, sem):
        return pltpu.make_async_copy(hbm, buf, sem)

    def part(hbm, buf, sem, c):
        block = pl.ds(c * GROUP, GROUP)
        return pltpu.make_async_copy(hbm.at[block], buf.at[block], sem.at[c])

    pairs = ((x_hbm, x_ref), (gain_hbm, gain_ref), (lens_hbm, lens_ref), (freq_hbm, freq_ref), (chosen_hbm, chosen_ref),
             (wq_hbm, wq), (wk_hbm, wk), (wv_hbm, wv))
    loads = [load(hbm, buf, wsem.at[i]) for i, (hbm, buf) in enumerate(pairs)]
    weights = loads[5:]
    for copy in loads:
        copy.start()
    for c in range(steps):
        part(k_hbm, kbuf, ksem, c).start()
        part(v_hbm, vbuf, vsem, c).start()
    for copy in loads[:5]:
        copy.wait()

    experts = 64
    sub = lax.broadcasted_iota(jnp.int32, (experts, rows), 0)
    hit = chosen_ref[0:1, :] == sub
    for k in range(1, chosen_ref.shape[0]):
        hit = hit | (chosen_ref[k:k + 1, :] == sub)
    used_col = jnp.max(hit.astype(F32), axis=1, keepdims=True)
    si = lax.broadcasted_iota(jnp.int32, (experts, 128), 0)
    li = lax.broadcasted_iota(jnp.int32, (experts, 128), 1)
    used_row = jnp.sum(jnp.where(si == li, used_col, 0.0), axis=0, keepdims=True)
    rank_col = jnp.sum(jnp.where(li < si, used_row, 0.0), axis=1, keepdims=True)
    pick = (rank_col == li.astype(F32)) & (used_col > 0.0)
    ids = jnp.sum(jnp.where(pick, si.astype(F32), 0.0), axis=0, keepdims=True)
    total = jnp.sum(used_row, axis=1, keepdims=True)
    lane1 = lax.broadcasted_iota(jnp.int32, (1, 128), 1)
    held = jnp.sum(jnp.where(lane1 < HELD, used_row, 0.0), axis=1, keepdims=True)
    list_ref[...] = jnp.where(lane1 == 127, total, jnp.where(lane1 == 126, held, ids)).astype(jnp.int32)

    h = norm_rows(x_ref[...], gain_ref[...])

    row_id = lax.broadcasted_iota(jnp.int32, (rows, dim), 0)
    pos = jnp.zeros((rows, dim), F32)
    for b in range(rows):
        pos = jnp.where(row_id == b, lens_ref[b].astype(F32), pos)
    angle = pos * freq_ref[...]
    cos_t = jnp.cos(angle)
    lane = lax.broadcasted_iota(jnp.int32, (rows, dim), 1)
    sin_t = jnp.where(lane < dim // 2, -jnp.sin(angle), jnp.sin(angle))

    def rope(y):
        return y * cos_t + pltpu.roll(y, dim // 2, 1) * sin_t

    def project(copy, w):
        copy.wait()
        return jnp.dot(h, w[...], preferred_element_type=F32)

    q = project(weights[0], wq)
    k = project(weights[1], wk)
    v = project(weights[2], wv)
    for j in range(2):
        cols = slice(j * dim, (j + 1) * dim)
        qs[:, cols] = rope(q[:, cols]).astype(BF16).astype(F32)
        ks[:, cols] = rope(k[:, cols]).astype(BF16).astype(F32)
        vs[:, cols] = v[:, cols].astype(BF16).astype(F32)

    r16 = lax.broadcasted_iota(jnp.int32, (16, dim), 0)
    srow = lax.broadcasted_iota(jnp.int32, (16, slots2), 0)
    scol = lax.broadcasted_iota(jnp.int32, (16, slots2), 1)
    same_head = (srow % 2) == (scol % 2)
    slot = scol // 2

    def put_row(buf, new, b, p):
        tile = pl.ds(pl.multiple_of((p // 8) * 16, 16), 16)
        old = buf[b, tile, :].astype(F32)
        head = jnp.where(r16 % 2 == 0, new[pl.ds(b, 1), 0:dim], new[pl.ds(b, 1), dim:2 * dim])
        buf[b, tile, :] = jnp.where(r16 // 2 == p % 8, head, old).astype(BF16)

    for c in range(steps):
        part(k_hbm, kbuf, ksem, c).wait()
        part(v_hbm, vbuf, vsem, c).wait()
        qblocks = []
        limit = jnp.zeros((16, slots2), jnp.int32)
        for j in range(GROUP):
            b = c * GROUP + j
            p = lens_ref[b]
            put_row(kbuf, ks, b, p)
            put_row(vbuf, vs, b, p)
            limit = jnp.where(srow // 2 == j, p, limit)
            qblocks.append(jnp.where(r16 == 2 * j, qs[b:b + 1, 0:dim], jnp.where(r16 == 2 * j + 1, qs[b:b + 1, dim:2 * dim], 0.0)))
        score = jnp.zeros((16, slots2), F32)
        for j in range(0, GROUP, 2):
            b = c * GROUP + j
            lhs = jnp.concatenate([qblocks[j], qblocks[j + 1]], axis=1).astype(BF16)
            rhs = jnp.concatenate([kbuf[b], kbuf[b + 1]], axis=1)
            score = score + lax.dot_general(lhs, rhs, NT, preferred_element_type=F32)
        score = score * (dim ** -0.5)
        valid = same_head & (slot <= limit)
        score = jnp.where(valid, score, MASK_FILL)
        top = jnp.max(score, axis=1, keepdims=True)
        e = jnp.where(valid, jnp.exp(score - top), 0.0)
        w = (e / jnp.sum(e, axis=1, keepdims=True)).astype(BF16)
        out = jnp.zeros((16, dim), F32)
        for j in range(0, GROUP, 2):
            b = c * GROUP + j
            rhs = jnp.concatenate([vbuf[b], vbuf[b + 1]], axis=1)
            both = jnp.dot(w, rhs, preferred_element_type=F32)
            out = jnp.where(r16 // 2 == j, both[:, 0:dim], out)
            out = jnp.where(r16 // 2 == j + 1, both[:, dim:2 * dim], out)
        os[c * 16:(c + 1) * 16, :] = out
        part(kbuf, ko_hbm, kosem, c).start()
        part(vbuf, vo_hbm, vosem, c).start()

    heads_ref[...] = jnp.concatenate([os[pl.ds(0, rows, stride=2), :], os[pl.ds(1, rows, stride=2), :]], axis=1).astype(BF16)
    for c in range(steps):
        part(kbuf, ko_hbm, kosem, c).wait()
        part(vbuf, vo_hbm, vosem, c).wait()


def attention(x, lens, chosen_t, gain, freq, wq, wk, wv, k_cache, v_cache):
    rows, width = x.shape
    steps = rows // GROUP
    return pl.pallas_call(
        attention_kernel,
        name="attention",
        out_shape=(
            pltpu.VMEM((rows, 256), BF16),
            pltpu.VMEM((1, 128), jnp.int32),
            jax.ShapeDtypeStruct(k_cache.shape, BF16),
            jax.ShapeDtypeStruct(v_cache.shape, BF16),
        ),
        in_specs=[ANY] * 10,
        out_specs=(VMEM, VMEM, ANY, ANY),
        scratch_shapes=[
            pltpu.VMEM(x.shape, BF16), pltpu.SMEM(lens.shape, jnp.int32), pltpu.VMEM(chosen_t.shape, jnp.int32),
            pltpu.VMEM(gain.shape, BF16), pltpu.VMEM(freq.shape, F32),
            pltpu.VMEM(wq.shape, BF16), pltpu.VMEM(wk.shape, BF16), pltpu.VMEM(wv.shape, BF16),
            pltpu.VMEM(k_cache.shape, BF16), pltpu.VMEM(v_cache.shape, BF16),
            pltpu.VMEM((rows, 256), F32), pltpu.VMEM((rows, 256), F32), pltpu.VMEM((rows, 256), F32),
            pltpu.VMEM((2 * rows, 128), F32),
            pltpu.SemaphoreType.DMA((8,)),
            pltpu.SemaphoreType.DMA((steps,)), pltpu.SemaphoreType.DMA((steps,)),
            pltpu.SemaphoreType.DMA((steps,)), pltpu.SemaphoreType.DMA((steps,)),
        ],
        compiler_params=pltpu.CompilerParams(vmem_limit_bytes=16 * 1024 * 1024),
    )(*in_hbm(x, lens, chosen_t, gain, freq, wq, wk, wv, k_cache, v_cache))


ORDER = (6, 2, 4, 7, 3, 5, 1)


def sum_kernel(n_ahead, project, *refs):
    if project:
        heads_ref, wo, *refs = refs
    else:
        part_ref, *refs = refs
    base_ref, *refs = refs
    ahead_hbm, (out_ref, *ahead), (inbox, piece, sems, *refs) = refs[:n_ahead], refs[n_ahead:2 * n_ahead + 1], refs[2 * n_ahead + 1:]
    me = lax.axis_index("tp")
    core, xx, yy = lax.rem(me, 2), lax.rem(me // 2, 2), me // 4
    cols = base_ref.shape[1] // 8

    def peer(m):
        return (1 - yy if m & 4 else yy) * 4 + (1 - xx if m & 2 else xx) * 2 + (1 - core if m & 1 else core)

    def columns(j):
        return pl.ds(pl.multiple_of(j * cols, cols), cols)

    def send(src, dst, m, phase):
        return pltpu.make_async_remote_copy(
            src_ref=src, dst_ref=dst, send_sem=sems.at[phase, m], recv_sem=sems.at[phase + 1, m],
            device_id={"tp": peer(m)}, device_id_type=pl.DeviceIdType.MESH)

    barrier = pltpu.get_barrier_semaphore()
    for m in ORDER:
        pl.semaphore_signal(barrier, inc=1, device_id={"tp": peer(m)}, device_id_type=pl.DeviceIdType.MESH)
    loads = []
    if project:
        part_ref, load_sems = refs
        loads = [pltpu.make_async_copy(src.at[pl.ds(e, 2)], dst.at[pl.ds(e, 2)], load_sems.at[m, e // 2])
                 for e in range(0, HELD, 2) for m, (src, dst) in enumerate(zip(ahead_hbm, ahead))]
        for load in loads:
            load.start()
        for j in range(0, base_ref.shape[1], cols):
            part_ref[:, j:j + cols] = jnp.dot(heads_ref[...], wo[:, j:j + cols], preferred_element_type=F32)
    pl.semaphore_wait(barrier, len(ORDER))

    first = {m: send(part_ref.at[:, columns(peer(m))], inbox.at[m - 1], m, 0) for m in ORDER}
    for m in ORDER:
        first[m].start()
    total = part_ref[:, columns(me)]
    for m in (1, 2, 4, 3, 5, 6, 7):
        first[m].wait_recv()
        total = total + inbox[m - 1]
    piece[...] = (base_ref[:, columns(me)].astype(F32) + total).astype(BF16)
    second = [send(piece, out_ref.at[:, columns(me)], m, 2) for m in ORDER]
    for copy in second:
        copy.start()
    out_ref[:, columns(me)] = piece[...]
    for m in ORDER:
        first[m].wait_send()
    for copy in second:
        copy.wait()
    for load in loads:
        load.wait()


def add_sum(partial, base, collective_id, ahead=()):
    rows, width = base.shape
    project = len(partial) == 2
    scratch = [pltpu.VMEM((7, rows, width // 8), F32), pltpu.VMEM((rows, width // 8), BF16), pltpu.SemaphoreType.DMA((4, 8))]
    if project:
        scratch += [pltpu.VMEM((rows, width), F32), pltpu.SemaphoreType.DMA((3, HELD // 2))]
    return pl.pallas_call(
        functools.partial(sum_kernel, len(ahead), project),
        name="add_sum",
        out_shape=[pltpu.VMEM(base.shape, BF16)] + [pltpu.VMEM((HELD, *a.shape[1:]), a.dtype) for a in ahead],
        in_specs=[VMEM] * (len(partial) + 1) + [ANY] * len(ahead),
        out_specs=[VMEM] * (1 + len(ahead)),
        scratch_shapes=scratch,
        compiler_params=pltpu.CompilerParams(collective_id=collective_id, has_side_effects=True, vmem_limit_bytes=4 * 1024 * 1024),
    )(*partial, base, *in_hbm(*ahead))


def experts_kernel(list_ref, x_ref, chosen_ref, gain_ref, wr_ref, held_g, held_u, held_d, gate_hbm, up_hbm, down_hbm, out_ref,
                   gates, h_ref, g_ref, u_ref, hg_ref, hu_ref, ring_g, ring_u, ring_d, sem):
    rows, width = x_ref.shape
    held, count = list_ref[0, 126], list_ref[0, 127]
    rest = count - held

    def fetch(i, go):
        slot = lax.rem(i, RING)
        e = list_ref[0, held + i]
        for m, (hbm, ring) in enumerate(((gate_hbm, ring_g), (up_hbm, ring_u), (down_hbm, ring_d))):
            copy = pltpu.make_async_copy(hbm.at[e], ring.at[slot], sem.at[m, slot])
            if go:
                copy.start()
            else:
                copy.wait()

    for i in range(RING - 2):
        @pl.when(i < rest)
        def _():
            fetch(i, True)

    h = norm_rows(x_ref[...], gain_ref[...])
    h_ref[...] = h
    logits = lax.dot_general(wr_ref[...], h, NT, preferred_element_type=F32)
    experts = logits.shape[0]
    sub = lax.broadcasted_iota(jnp.int32, (experts, rows), 0)
    hit = chosen_ref[0:1, :] == sub
    for k in range(1, chosen_ref.shape[0]):
        hit = hit | (chosen_ref[k:k + 1, :] == sub)
    top = jnp.max(jnp.where(hit, logits, MASK_FILL), axis=0, keepdims=True)
    e = jnp.where(hit, jnp.exp(jnp.where(hit, logits - top, 0.0)), 0.0)
    gates[...] = (e / jnp.sum(e, axis=0, keepdims=True)).T
    out_ref[...] = jnp.zeros_like(out_ref)
    lane = lax.broadcasted_iota(jnp.int32, (rows, experts), 1)
    tile = 256

    def inner(e, g, u):
        column = jnp.sum(jnp.where(lane == e, gates[...], 0.0), axis=1, keepdims=True)
        return (column * jax.nn.silu(g[...]) * u[...]).astype(BF16)

    def wide(gate, up):
        g = u = None
        for t in range(0, width, tile):
            hk = h_ref[:, t:t + tile]
            gt = lax.dot_general(hk, gate(t), NT, preferred_element_type=F32)
            ut = lax.dot_general(up(t), hk, NT, preferred_element_type=F32)
            g, u = (gt, ut) if g is None else (g + gt, u + ut)
        return g, u.T

    def narrow(z, down):
        for t in range(0, width, tile):
            out_ref[:, t:t + tile] += jnp.dot(z, down(t), preferred_element_type=F32)

    def views(refs, index):
        return [lambda t, ref=ref: ref[index, :, t:t + tile] for ref in refs]

    def step_held(i):
        before = list_ref[0, jnp.maximum(i - 1, 0)]
        z = inner(before, hg_ref, hu_ref)
        g, u = wide(*views((held_g, held_u), list_ref[0, i]))
        narrow(z, *views((held_d,), before))
        hg_ref[...], hu_ref[...] = g, u

    def step_rest(i, carry):
        share, done = carry

        @pl.when(i + RING - 2 < rest)
        def _():
            fetch(i + RING - 2, True)

        @pl.when(i < rest)
        def _():
            fetch(i, False)

        z = inner(list_ref[0, jnp.maximum(held + i - 1, 0)], g_ref, u_ref)
        g, u = wide(*views((ring_g, ring_u), lax.rem(i, RING)))
        narrow(z, *views((ring_d,), lax.rem(i + RING - 1, RING)))
        g_ref[...], u_ref[...] = g, u

        share = share + held
        more = (share >= rest) & (done < held)

        @pl.when(more)
        def _():
            step_held(done)

        return jnp.where(more, share - rest, share), jnp.where(more, done + 1, done)

    for ref in (g_ref, u_ref, hg_ref, hu_ref):
        ref[...] = jnp.zeros_like(ref)
    ring_d[RING - 1] = jnp.zeros(ring_d.shape[1:], BF16)
    steps = jnp.where(rest > 0, rest + 1, 0)
    _, done = lax.fori_loop(0, steps, step_rest, (jnp.int32(0), jnp.int32(0)))

    def remaining(i, carry):
        step_held(i)
        return carry

    lax.fori_loop(done, held, remaining, 0)

    @pl.when(held > 0)
    def _():
        before = list_ref[0, held - 1]
        narrow(inner(before, hg_ref, hu_ref), *views((held_d,), before))


def experts_part(ids, x1, chosen_t, gain, wr_t, held, gate_t, up_t, down):
    rows, width = x1.shape
    n_experts, hidden = gate_t.shape[:2]
    return pl.pallas_call(
        experts_kernel,
        name="experts",
        out_shape=pltpu.VMEM((rows, width), F32),
        in_specs=[SMEM, VMEM, VMEM, VMEM, VMEM, VMEM, VMEM, VMEM, ANY, ANY, ANY],
        out_specs=VMEM,
        scratch_shapes=[
            pltpu.VMEM((rows, n_experts), F32), pltpu.VMEM((rows, width), BF16),
            pltpu.VMEM((rows, hidden), F32), pltpu.VMEM((rows, hidden), F32),
            pltpu.VMEM((rows, hidden), F32), pltpu.VMEM((rows, hidden), F32),
            pltpu.VMEM((RING, hidden, width), BF16), pltpu.VMEM((RING, hidden, width), BF16), pltpu.VMEM((RING, hidden, width), BF16),
            pltpu.SemaphoreType.DMA((3, RING)),
        ],
        compiler_params=pltpu.CompilerParams(vmem_limit_bytes=12 * 1024 * 1024),
    )(ids, x1, chosen_t, gain, wr_t, *held, *in_hbm(gate_t, up_t, down))


def solution(mesh):
    cache_spec = P("dp", None, "tp", None)
    in_specs = (P("dp", None), cache_spec, cache_spec, P("dp"), P("dp", None), P(None), P(None, "tp"), P(None, "tp"), P(None, "tp"), P("tp", None), P(None), P(None, None), P(None, None, "tp"), P(None, None, "tp"), P(None, "tp", None))
    out_specs = (P("dp", None), cache_spec, cache_spec)
    freq = (np.float32(ROPE_THETA) ** (-np.arange(0, 128, 2, dtype=np.float32) / np.float32(128))).astype(np.float32)
    freq = np.concatenate([freq, freq])[None, :]

    def layer_shard(hidden_in, k_cache, v_cache, seq_lens, chosen, g_attn, w_q, w_k, w_v, w_o, g_moe, w_router, w_gate, w_up, w_down):
        rows, slots, kv_heads, dim = k_cache.shape
        width = hidden_in.shape[1]
        chosen_t = chosen.T
        flat = (rows, slots * kv_heads, dim)
        heads, ids, k_next, v_next = attention(
            hidden_in, seq_lens, chosen_t, g_attn.reshape(width // 128, 128), jnp.asarray(freq), w_q, w_k, w_v,
            k_cache.reshape(flat), v_cache.reshape(flat))
        experts = (jnp.swapaxes(w_gate, 1, 2), jnp.swapaxes(w_up, 1, 2), w_down)
        x1, *held = add_sum((heads, w_o), hidden_in, 1, experts)
        moe = experts_part(ids, x1, chosen_t, g_moe.reshape(width // 128, 128), w_router.T, held, *experts)
        out, = add_sum((moe,), x1, 2)
        return out, k_next.reshape(k_cache.shape), v_next.reshape(v_cache.shape)

    return jax.shard_map(layer_shard, mesh=mesh, in_specs=in_specs, out_specs=out_specs, check_vma=False)
```

```python
import functools

import jax
import jax.numpy as jnp
import numpy as np
from jax import lax
from jax.experimental import pallas as pl
from jax.experimental.pallas import tpu as pltpu
from jax.sharding import PartitionSpec as P

EPSILON = 1e-5
ROPE_THETA = 1000000.0
MASK_FILL = -1e30
F32 = jnp.float32
BF16 = jnp.bfloat16
ANY = pl.BlockSpec(memory_space=pltpu.HBM)
VMEM = pl.BlockSpec(memory_space=pltpu.VMEM)
SMEM = pl.BlockSpec(memory_space=pltpu.SMEM)
NT = (((1,), (1,)), ((), ()))


def in_hbm(*arrays):
    return [pltpu.with_memory_space_constraint(a, pltpu.HBM) for a in arrays]


GROUP = 8
RING = 6
HELD = 14


def norm_rows(x, gain):
    x32 = x.astype(F32)
    scale = lax.rsqrt(jnp.mean(x32 * x32, axis=-1, keepdims=True) + EPSILON)
    gain32 = gain.astype(F32)
    gain_row = jnp.concatenate([gain32[i:i + 1, :] for i in range(gain.shape[0])], axis=1)
    return (x32 * scale * gain_row).astype(BF16)


def attention_kernel(x_hbm, lens_hbm, chosen_hbm, gain_hbm, freq_hbm, wq_hbm, wk_hbm, wv_hbm, k_hbm, v_hbm,
                     heads_ref, list_ref, ko_hbm, vo_hbm,
                     x_ref, lens_ref, chosen_ref, gain_ref, freq_ref, wq, wk, wv, kbuf, vbuf, qs, ks, vs, os,
                     wsem, ksem, vsem, kosem, vosem):
    rows, width = x_ref.shape
    slots2, dim = kbuf.shape[1], kbuf.shape[2]
    steps = rows // GROUP

    def load(hbm, buf, sem):
        return pltpu.make_async_copy(hbm, buf, sem)

    def part(hbm, buf, sem, c):
        block = pl.ds(c * GROUP, GROUP)
        return pltpu.make_async_copy(hbm.at[block], buf.at[block], sem.at[c])

    pairs = ((x_hbm, x_ref), (gain_hbm, gain_ref), (lens_hbm, lens_ref), (freq_hbm, freq_ref), (chosen_hbm, chosen_ref),
             (wq_hbm, wq), (wk_hbm, wk), (wv_hbm, wv))
    loads = [load(hbm, buf, wsem.at[i]) for i, (hbm, buf) in enumerate(pairs)]
    weights = loads[5:]
    for copy in loads:
        copy.start()
    for c in range(steps):
        part(k_hbm, kbuf, ksem, c).start()
        part(v_hbm, vbuf, vsem, c).start()
    for copy in loads[:5]:
        copy.wait()

    experts = 64
    sub = lax.broadcasted_iota(jnp.int32, (experts, rows), 0)
    hit = chosen_ref[0:1, :] == sub
    for k in range(1, chosen_ref.shape[0]):
        hit = hit | (chosen_ref[k:k + 1, :] == sub)
    used_col = jnp.max(hit.astype(F32), axis=1, keepdims=True)
    si = lax.broadcasted_iota(jnp.int32, (experts, 128), 0)
    li = lax.broadcasted_iota(jnp.int32, (experts, 128), 1)
    used_row = jnp.sum(jnp.where(si == li, used_col, 0.0), axis=0, keepdims=True)
    rank_col = jnp.sum(jnp.where(li < si, used_row, 0.0), axis=1, keepdims=True)
    pick = (rank_col == li.astype(F32)) & (used_col > 0.0)
    ids = jnp.sum(jnp.where(pick, si.astype(F32), 0.0), axis=0, keepdims=True)
    total = jnp.sum(used_row, axis=1, keepdims=True)
    lane1 = lax.broadcasted_iota(jnp.int32, (1, 128), 1)
    held = jnp.sum(jnp.where(lane1 < HELD, used_row, 0.0), axis=1, keepdims=True)
    list_ref[...] = jnp.where(lane1 == 127, total, jnp.where(lane1 == 126, held, ids)).astype(jnp.int32)

    h = norm_rows(x_ref[...], gain_ref[...])

    row_id = lax.broadcasted_iota(jnp.int32, (rows, dim), 0)
    pos = jnp.zeros((rows, dim), F32)
    for b in range(rows):
        pos = jnp.where(row_id == b, lens_ref[b].astype(F32), pos)
    angle = pos * freq_ref[...]
    cos_t = jnp.cos(angle)
    lane = lax.broadcasted_iota(jnp.int32, (rows, dim), 1)
    sin_t = jnp.where(lane < dim // 2, -jnp.sin(angle), jnp.sin(angle))

    def rope(y):
        return y * cos_t + pltpu.roll(y, dim // 2, 1) * sin_t

    def project(copy, w):
        copy.wait()
        return jnp.dot(h, w[...], preferred_element_type=F32)

    q = project(weights[0], wq)
    k = project(weights[1], wk)
    v = project(weights[2], wv)
    for j in range(2):
        cols = slice(j * dim, (j + 1) * dim)
        qs[:, cols] = rope(q[:, cols]).astype(BF16).astype(F32)
        ks[:, cols] = rope(k[:, cols]).astype(BF16).astype(F32)
        vs[:, cols] = v[:, cols].astype(BF16).astype(F32)

    r16 = lax.broadcasted_iota(jnp.int32, (16, dim), 0)
    srow = lax.broadcasted_iota(jnp.int32, (16, slots2), 0)
    scol = lax.broadcasted_iota(jnp.int32, (16, slots2), 1)
    same_head = (srow % 2) == (scol % 2)
    slot = scol // 2

    def put_row(buf, new, b, p):
        tile = pl.ds(pl.multiple_of((p // 8) * 16, 16), 16)
        old = buf[b, tile, :].astype(F32)
        head = jnp.where(r16 % 2 == 0, new[pl.ds(b, 1), 0:dim], new[pl.ds(b, 1), dim:2 * dim])
        buf[b, tile, :] = jnp.where(r16 // 2 == p % 8, head, old).astype(BF16)

    for c in range(steps):
        part(k_hbm, kbuf, ksem, c).wait()
        part(v_hbm, vbuf, vsem, c).wait()
        qblocks = []
        limit = jnp.zeros((16, slots2), jnp.int32)
        for j in range(GROUP):
            b = c * GROUP + j
            p = lens_ref[b]
            put_row(kbuf, ks, b, p)
            put_row(vbuf, vs, b, p)
            limit = jnp.where(srow // 2 == j, p, limit)
            qblocks.append(jnp.where(r16 == 2 * j, qs[b:b + 1, 0:dim], jnp.where(r16 == 2 * j + 1, qs[b:b + 1, dim:2 * dim], 0.0)))
        score = jnp.zeros((16, slots2), F32)
        for j in range(0, GROUP, 2):
            b = c * GROUP + j
            lhs = jnp.concatenate([qblocks[j], qblocks[j + 1]], axis=1).astype(BF16)
            rhs = jnp.concatenate([kbuf[b], kbuf[b + 1]], axis=1)
            score = score + lax.dot_general(lhs, rhs, NT, preferred_element_type=F32)
        score = score * (dim ** -0.5)
        valid = same_head & (slot <= limit)
        score = jnp.where(valid, score, MASK_FILL)
        top = jnp.max(score, axis=1, keepdims=True)
        e = jnp.where(valid, jnp.exp(score - top), 0.0)
        w = (e / jnp.sum(e, axis=1, keepdims=True)).astype(BF16)
        out = jnp.zeros((16, dim), F32)
        for j in range(0, GROUP, 2):
            b = c * GROUP + j
            rhs = jnp.concatenate([vbuf[b], vbuf[b + 1]], axis=1)
            both = jnp.dot(w, rhs, preferred_element_type=F32)
            out = jnp.where(r16 // 2 == j, both[:, 0:dim], out)
            out = jnp.where(r16 // 2 == j + 1, both[:, dim:2 * dim], out)
        os[c * 16:(c + 1) * 16, :] = out
        part(kbuf, ko_hbm, kosem, c).start()
        part(vbuf, vo_hbm, vosem, c).start()

    heads_ref[...] = jnp.concatenate([os[pl.ds(0, rows, stride=2), :], os[pl.ds(1, rows, stride=2), :]], axis=1).astype(BF16)
    for c in range(steps):
        part(kbuf, ko_hbm, kosem, c).wait()
        part(vbuf, vo_hbm, vosem, c).wait()


def attention(x, lens, chosen_t, gain, freq, wq, wk, wv, k_cache, v_cache):
    rows, width = x.shape
    steps = rows // GROUP
    return pl.pallas_call(
        attention_kernel,
        name="attention",
        out_shape=(
            pltpu.VMEM((rows, 256), BF16),
            pltpu.VMEM((1, 128), jnp.int32),
            jax.ShapeDtypeStruct(k_cache.shape, BF16),
            jax.ShapeDtypeStruct(v_cache.shape, BF16),
        ),
        in_specs=[ANY] * 10,
        out_specs=(VMEM, VMEM, ANY, ANY),
        scratch_shapes=[
            pltpu.VMEM(x.shape, BF16), pltpu.SMEM(lens.shape, jnp.int32), pltpu.VMEM(chosen_t.shape, jnp.int32),
            pltpu.VMEM(gain.shape, BF16), pltpu.VMEM(freq.shape, F32),
            pltpu.VMEM(wq.shape, BF16), pltpu.VMEM(wk.shape, BF16), pltpu.VMEM(wv.shape, BF16),
            pltpu.VMEM(k_cache.shape, BF16), pltpu.VMEM(v_cache.shape, BF16),
            pltpu.VMEM((rows, 256), F32), pltpu.VMEM((rows, 256), F32), pltpu.VMEM((rows, 256), F32),
            pltpu.VMEM((2 * rows, 128), F32),
            pltpu.SemaphoreType.DMA((8,)),
            pltpu.SemaphoreType.DMA((steps,)), pltpu.SemaphoreType.DMA((steps,)),
            pltpu.SemaphoreType.DMA((steps,)), pltpu.SemaphoreType.DMA((steps,)),
        ],
        compiler_params=pltpu.CompilerParams(vmem_limit_bytes=16 * 1024 * 1024),
    )(*in_hbm(x, lens, chosen_t, gain, freq, wq, wk, wv, k_cache, v_cache))


ORDER = (6, 2, 4, 7, 3, 5, 1)


def sum_kernel(n_ahead, project, *refs):
    if project:
        heads_ref, wo, *refs = refs
    else:
        part_ref, *refs = refs
    base_ref, *refs = refs
    ahead_hbm, (out_ref, *ahead), (inbox, piece, sems, *refs) = refs[:n_ahead], refs[n_ahead:2 * n_ahead + 1], refs[2 * n_ahead + 1:]
    me = lax.axis_index("tp")
    core, xx, yy = lax.rem(me, 2), lax.rem(me // 2, 2), me // 4
    cols = base_ref.shape[1] // 8

    def peer(m):
        return (1 - yy if m & 4 else yy) * 4 + (1 - xx if m & 2 else xx) * 2 + (1 - core if m & 1 else core)

    def columns(j):
        return pl.ds(pl.multiple_of(j * cols, cols), cols)

    def send(src, dst, m, phase):
        return pltpu.make_async_remote_copy(
            src_ref=src, dst_ref=dst, send_sem=sems.at[phase, m], recv_sem=sems.at[phase + 1, m],
            device_id={"tp": peer(m)}, device_id_type=pl.DeviceIdType.MESH)

    barrier = pltpu.get_barrier_semaphore()
    for m in ORDER:
        pl.semaphore_signal(barrier, inc=1, device_id={"tp": peer(m)}, device_id_type=pl.DeviceIdType.MESH)
    loads = []
    if project:
        part_ref, load_sems = refs
        loads = [pltpu.make_async_copy(src.at[pl.ds(e, 2)], dst.at[pl.ds(e, 2)], load_sems.at[m, e // 2])
                 for e in range(0, HELD, 2) for m, (src, dst) in enumerate(zip(ahead_hbm, ahead))]
        for load in loads:
            load.start()
        for j in range(0, base_ref.shape[1], cols):
            part_ref[:, j:j + cols] = jnp.dot(heads_ref[...], wo[:, j:j + cols], preferred_element_type=F32)
    pl.semaphore_wait(barrier, len(ORDER))

    first = {m: send(part_ref.at[:, columns(peer(m))], inbox.at[m - 1], m, 0) for m in ORDER}
    for m in ORDER:
        first[m].start()
    total = part_ref[:, columns(me)]
    for m in (1, 2, 4, 3, 5, 6, 7):
        first[m].wait_recv()
        total = total + inbox[m - 1]
    piece[...] = (base_ref[:, columns(me)].astype(F32) + total).astype(BF16)
    second = [send(piece, out_ref.at[:, columns(me)], m, 2) for m in ORDER]
    for copy in second:
        copy.start()
    out_ref[:, columns(me)] = piece[...]
    for m in ORDER:
        first[m].wait_send()
    for copy in second:
        copy.wait()
    for load in loads:
        load.wait()


def add_sum(partial, base, collective_id, ahead=()):
    rows, width = base.shape
    project = len(partial) == 2
    scratch = [pltpu.VMEM((7, rows, width // 8), F32), pltpu.VMEM((rows, width // 8), BF16), pltpu.SemaphoreType.DMA((4, 8))]
    if project:
        scratch += [pltpu.VMEM((rows, width), F32), pltpu.SemaphoreType.DMA((3, HELD // 2))]
    return pl.pallas_call(
        functools.partial(sum_kernel, len(ahead), project),
        name="add_sum",
        out_shape=[pltpu.VMEM(base.shape, BF16)] + [pltpu.VMEM((HELD, *a.shape[1:]), a.dtype) for a in ahead],
        in_specs=[VMEM] * (len(partial) + 1) + [ANY] * len(ahead),
        out_specs=[VMEM] * (1 + len(ahead)),
        scratch_shapes=scratch,
        compiler_params=pltpu.CompilerParams(collective_id=collective_id, has_side_effects=True, vmem_limit_bytes=4 * 1024 * 1024),
    )(*partial, base, *in_hbm(*ahead))


def experts_kernel(list_ref, x_ref, chosen_ref, gain_ref, wr_ref, held_g, held_u, held_d, gate_hbm, up_hbm, down_hbm, out_ref,
                   gates, h_ref, ring_g, ring_u, ring_d, sem):
    rows, width = x_ref.shape
    held, count = list_ref[0, 126], list_ref[0, 127]
    rest = count - held

    def fetch(i, go):
        slot = lax.rem(i, RING)
        e = list_ref[0, held + i]
        for m, (hbm, ring) in enumerate(((gate_hbm, ring_g), (up_hbm, ring_u), (down_hbm, ring_d))):
            copy = pltpu.make_async_copy(hbm.at[e], ring.at[slot], sem.at[m, slot])
            if go:
                copy.start()
            else:
                copy.wait()

    def fetch_pair(p, go):
        for i in (2 * p, 2 * p + 1):
            @pl.when(i < rest)
            def _():
                fetch(i, go)

    for p in range(RING // 2 - 1):
        fetch_pair(p, True)

    h = norm_rows(x_ref[...], gain_ref[...])
    h_ref[...] = h
    logits = lax.dot_general(wr_ref[...], h, NT, preferred_element_type=F32)
    experts = logits.shape[0]
    sub = lax.broadcasted_iota(jnp.int32, (experts, rows), 0)
    hit = chosen_ref[0:1, :] == sub
    for k in range(1, chosen_ref.shape[0]):
        hit = hit | (chosen_ref[k:k + 1, :] == sub)
    top = jnp.max(jnp.where(hit, logits, MASK_FILL), axis=0, keepdims=True)
    e = jnp.where(hit, jnp.exp(jnp.where(hit, logits - top, 0.0)), 0.0)
    gates[...] = (e / jnp.sum(e, axis=0, keepdims=True)).T
    out_ref[...] = jnp.zeros_like(out_ref)
    lane = lax.broadcasted_iota(jnp.int32, (rows, experts), 1)
    tile = 512

    def wide(e, gate, up, weight):
        g = u = None
        for t in range(0, width, tile):
            hk = h_ref[:, t:t + tile]
            gt = lax.dot_general(gate[:, t:t + tile], hk, NT, preferred_element_type=F32)
            ut = lax.dot_general(hk, up[:, t:t + tile], NT, preferred_element_type=F32)
            g, u = (gt, ut) if g is None else (g + gt, u + ut)
        column = weight * jnp.sum(jnp.where(lane == e, gates[...], 0.0), axis=1, keepdims=True)
        return (column * jax.nn.silu(g.T) * u).astype(BF16)

    def narrow(z, down):
        for t in range(0, width, tile):
            out_ref[:, t:t + tile] += jnp.dot(z, down[:, t:t + tile], preferred_element_type=F32)

    def block(items):
        zs = [wide(e, gate, up, weight) for e, gate, up, _, weight in items]
        for z, (_, _, _, down, _) in zip(zs, items):
            narrow(z, down)

    def held_item(j):
        e = list_ref[0, j]
        return e, held_g.at[e], held_u.at[e], held_d.at[e], 1.0

    def ring_item(i):
        at = jnp.minimum(i, rest - 1)
        slot = lax.rem(at, RING)
        weight = jnp.where(i < rest, 1.0, 0.0)
        return list_ref[0, held + at], ring_g.at[slot], ring_u.at[slot], ring_d.at[slot], weight

    def step(p, done):
        fetch_pair(p + RING // 2 - 1, True)
        fetch_pair(p, False)

        @pl.when(done < held)
        def _():
            block([ring_item(2 * p), ring_item(2 * p + 1), held_item(done)])

        @pl.when(done >= held)
        def _():
            block([ring_item(2 * p), ring_item(2 * p + 1)])

        return jnp.minimum(done + 1, held)

    def remaining(j, carry):
        block([held_item(j)])
        return carry

    done = lax.fori_loop(0, (rest + 1) // 2, step, 0)
    lax.fori_loop(done, held, remaining, 0)


def experts_part(ids, x1, chosen_t, gain, wr_t, held, gate_t, up_t, down):
    rows, width = x1.shape
    n_experts, hidden = gate_t.shape[:2]
    return pl.pallas_call(
        experts_kernel,
        name="experts",
        out_shape=pltpu.VMEM((rows, width), F32),
        in_specs=[SMEM, VMEM, VMEM, VMEM, VMEM, VMEM, VMEM, VMEM, ANY, ANY, ANY],
        out_specs=VMEM,
        scratch_shapes=[
            pltpu.VMEM((rows, n_experts), F32), pltpu.VMEM((rows, width), BF16),
            pltpu.VMEM((RING, hidden, width), BF16), pltpu.VMEM((RING, hidden, width), BF16), pltpu.VMEM((RING, hidden, width), BF16),
            pltpu.SemaphoreType.DMA((3, RING)),
        ],
        compiler_params=pltpu.CompilerParams(vmem_limit_bytes=15 * 1024 * 1024),
    )(ids, x1, chosen_t, gain, wr_t, *held, *in_hbm(gate_t, up_t, down))


def solution(mesh):
    cache_spec = P("dp", None, "tp", None)
    in_specs = (P("dp", None), cache_spec, cache_spec, P("dp"), P("dp", None), P(None), P(None, "tp"), P(None, "tp"), P(None, "tp"), P("tp", None), P(None), P(None, None), P(None, None, "tp"), P(None, None, "tp"), P(None, "tp", None))
    out_specs = (P("dp", None), cache_spec, cache_spec)
    freq = (np.float32(ROPE_THETA) ** (-np.arange(0, 128, 2, dtype=np.float32) / np.float32(128))).astype(np.float32)
    freq = np.concatenate([freq, freq])[None, :]

    def layer_shard(hidden_in, k_cache, v_cache, seq_lens, chosen, g_attn, w_q, w_k, w_v, w_o, g_moe, w_router, w_gate, w_up, w_down):
        rows, slots, kv_heads, dim = k_cache.shape
        width = hidden_in.shape[1]
        chosen_t = chosen.T
        flat = (rows, slots * kv_heads, dim)
        heads, ids, k_next, v_next = attention(
            hidden_in, seq_lens, chosen_t, g_attn.reshape(width // 128, 128), jnp.asarray(freq), w_q, w_k, w_v,
            k_cache.reshape(flat), v_cache.reshape(flat))
        experts = (jnp.swapaxes(w_gate, 1, 2), jnp.swapaxes(w_up, 1, 2), w_down)
        x1, *held = add_sum((heads, w_o), hidden_in, 1, experts)
        moe = experts_part(ids, x1, chosen_t, g_moe.reshape(width // 128, 128), w_router.T, held, *experts)
        out, = add_sum((moe,), x1, 2)
        return out, k_next.reshape(k_cache.shape), v_next.reshape(v_cache.shape)

    return jax.shard_map(layer_shard, mesh=mesh, in_specs=in_specs, out_specs=out_specs, check_vma=False)
```

```python
import functools

import jax
import jax.numpy as jnp
import numpy as np
from jax import lax
from jax.experimental import pallas as pl
from jax.experimental.pallas import tpu as pltpu
from jax.sharding import PartitionSpec as P

EPSILON = 1e-5
ROPE_THETA = 1000000.0
MASK_FILL = -1e30
F32 = jnp.float32
BF16 = jnp.bfloat16
ANY = pl.BlockSpec(memory_space=pltpu.HBM)
VMEM = pl.BlockSpec(memory_space=pltpu.VMEM)
SMEM = pl.BlockSpec(memory_space=pltpu.SMEM)
NT = (((1,), (1,)), ((), ()))


def in_hbm(*arrays):
    return [pltpu.with_memory_space_constraint(a, pltpu.HBM) for a in arrays]


GROUP = 8
RING = 6
HELD = 12


def norm_rows(x, gain):
    x32 = x.astype(F32)
    scale = lax.rsqrt(jnp.mean(x32 * x32, axis=-1, keepdims=True) + EPSILON)
    gain32 = gain.astype(F32)
    gain_row = jnp.concatenate([gain32[i:i + 1, :] for i in range(gain.shape[0])], axis=1)
    return (x32 * scale * gain_row).astype(BF16)


def attention_kernel(x_hbm, lens_hbm, chosen_hbm, gain_hbm, freq_hbm, wq_hbm, wk_hbm, wv_hbm, k_hbm, v_hbm,
                     heads_ref, list_ref, ko_hbm, vo_hbm,
                     x_ref, lens_ref, chosen_ref, gain_ref, freq_ref, wq, wk, wv, kbuf, vbuf, qs, ks, vs, os,
                     wsem, ksem, vsem, kosem, vosem):
    rows, width = x_ref.shape
    slots2, dim = kbuf.shape[1], kbuf.shape[2]
    steps = rows // GROUP

    def load(hbm, buf, sem):
        return pltpu.make_async_copy(hbm, buf, sem)

    def part(hbm, buf, sem, c):
        block = pl.ds(c * GROUP, GROUP)
        return pltpu.make_async_copy(hbm.at[block], buf.at[block], sem.at[c])

    pairs = ((x_hbm, x_ref), (gain_hbm, gain_ref), (lens_hbm, lens_ref), (freq_hbm, freq_ref), (chosen_hbm, chosen_ref),
             (wq_hbm, wq), (wk_hbm, wk), (wv_hbm, wv))
    loads = [load(hbm, buf, wsem.at[i]) for i, (hbm, buf) in enumerate(pairs)]
    weights = loads[5:]
    for copy in loads:
        copy.start()
    for c in range(steps):
        part(k_hbm, kbuf, ksem, c).start()
        part(v_hbm, vbuf, vsem, c).start()
    for copy in loads[:5]:
        copy.wait()

    experts = 64
    sub = lax.broadcasted_iota(jnp.int32, (experts, rows), 0)
    hit = chosen_ref[0:1, :] == sub
    for k in range(1, chosen_ref.shape[0]):
        hit = hit | (chosen_ref[k:k + 1, :] == sub)
    used_col = jnp.max(hit.astype(F32), axis=1, keepdims=True)
    si = lax.broadcasted_iota(jnp.int32, (experts, 128), 0)
    li = lax.broadcasted_iota(jnp.int32, (experts, 128), 1)
    used_row = jnp.sum(jnp.where(si == li, used_col, 0.0), axis=0, keepdims=True)
    rank_col = jnp.sum(jnp.where(li < si, used_row, 0.0), axis=1, keepdims=True)
    pick = (rank_col == li.astype(F32)) & (used_col > 0.0)
    ids = jnp.sum(jnp.where(pick, si.astype(F32), 0.0), axis=0, keepdims=True)
    total = jnp.sum(used_row, axis=1, keepdims=True)
    lane1 = lax.broadcasted_iota(jnp.int32, (1, 128), 1)
    held = jnp.sum(jnp.where(lane1 < HELD, used_row, 0.0), axis=1, keepdims=True)
    list_ref[...] = jnp.where(lane1 == 127, total, jnp.where(lane1 == 126, held, ids)).astype(jnp.int32)

    h = norm_rows(x_ref[...], gain_ref[...])

    row_id = lax.broadcasted_iota(jnp.int32, (rows, dim), 0)
    pos = jnp.zeros((rows, dim), F32)
    for b in range(rows):
        pos = jnp.where(row_id == b, lens_ref[b].astype(F32), pos)
    angle = pos * freq_ref[...]
    cos_t = jnp.cos(angle)
    lane = lax.broadcasted_iota(jnp.int32, (rows, dim), 1)
    sin_t = jnp.where(lane < dim // 2, -jnp.sin(angle), jnp.sin(angle))

    def rope(y):
        return y * cos_t + pltpu.roll(y, dim // 2, 1) * sin_t

    def project(copy, w):
        copy.wait()
        return jnp.dot(h, w[...], preferred_element_type=F32)

    q = project(weights[0], wq)
    k = project(weights[1], wk)
    v = project(weights[2], wv)
    for j in range(2):
        cols = slice(j * dim, (j + 1) * dim)
        qs[:, cols] = rope(q[:, cols]).astype(BF16).astype(F32)
        ks[:, cols] = rope(k[:, cols]).astype(BF16).astype(F32)
        vs[:, cols] = v[:, cols].astype(BF16).astype(F32)

    r16 = lax.broadcasted_iota(jnp.int32, (16, dim), 0)
    srow = lax.broadcasted_iota(jnp.int32, (16, slots2), 0)
    scol = lax.broadcasted_iota(jnp.int32, (16, slots2), 1)
    same_head = (srow % 2) == (scol % 2)
    slot = scol // 2

    def put_row(buf, new, b, p):
        tile = pl.ds(pl.multiple_of((p // 8) * 16, 16), 16)
        old = buf[b, tile, :].astype(F32)
        head = jnp.where(r16 % 2 == 0, new[pl.ds(b, 1), 0:dim], new[pl.ds(b, 1), dim:2 * dim])
        buf[b, tile, :] = jnp.where(r16 // 2 == p % 8, head, old).astype(BF16)

    def receive(c):
        part(k_hbm, kbuf, ksem, c).wait()
        part(v_hbm, vbuf, vsem, c).wait()
        for b in range(c * GROUP, (c + 1) * GROUP):
            put_row(kbuf, ks, b, lens_ref[b])
            put_row(vbuf, vs, b, lens_ref[b])

    def write(c):
        part(kbuf, ko_hbm, kosem, c).start()
        part(vbuf, vo_hbm, vosem, c).start()

    receive(0)
    for c in range(steps):
        if c + 1 < steps:
            receive(c + 1)
        if c == 0:
            write(0)
        qblocks = []
        limit = jnp.zeros((16, slots2), jnp.int32)
        for j in range(GROUP):
            b = c * GROUP + j
            p = lens_ref[b]
            limit = jnp.where(srow // 2 == j, p, limit)
            qblocks.append(jnp.where(r16 == 2 * j, qs[b:b + 1, 0:dim], jnp.where(r16 == 2 * j + 1, qs[b:b + 1, dim:2 * dim], 0.0)))
        score = jnp.zeros((16, slots2), F32)
        for j in range(0, GROUP, 2):
            b = c * GROUP + j
            lhs = jnp.concatenate([qblocks[j], qblocks[j + 1]], axis=1).astype(BF16)
            rhs = jnp.concatenate([kbuf[b], kbuf[b + 1]], axis=1)
            score = score + lax.dot_general(lhs, rhs, NT, preferred_element_type=F32)
        score = score * (dim ** -0.5)
        valid = same_head & (slot <= limit)
        score = jnp.where(valid, score, MASK_FILL)
        top = jnp.max(score, axis=1, keepdims=True)
        e = jnp.where(valid, jnp.exp(score - top), 0.0)
        w = (e / jnp.sum(e, axis=1, keepdims=True)).astype(BF16)
        out = jnp.zeros((16, dim), F32)
        for j in range(0, GROUP, 2):
            b = c * GROUP + j
            rhs = jnp.concatenate([vbuf[b], vbuf[b + 1]], axis=1)
            both = jnp.dot(w, rhs, preferred_element_type=F32)
            out = jnp.where(r16 // 2 == j, both[:, 0:dim], out)
            out = jnp.where(r16 // 2 == j + 1, both[:, dim:2 * dim], out)
        os[c * 16:(c + 1) * 16, :] = out
        if c + 1 < steps:
            write(c + 1)

    heads_ref[...] = jnp.concatenate([os[pl.ds(0, rows, stride=2), :], os[pl.ds(1, rows, stride=2), :]], axis=1).astype(BF16)
    for c in range(steps):
        part(kbuf, ko_hbm, kosem, c).wait()
        part(vbuf, vo_hbm, vosem, c).wait()


def attention(x, lens, chosen_t, gain, freq, wq, wk, wv, k_cache, v_cache):
    rows, width = x.shape
    steps = rows // GROUP
    return pl.pallas_call(
        attention_kernel,
        name="attention",
        out_shape=(
            pltpu.VMEM((rows, 256), BF16),
            pltpu.VMEM((1, 128), jnp.int32),
            jax.ShapeDtypeStruct(k_cache.shape, BF16),
            jax.ShapeDtypeStruct(v_cache.shape, BF16),
        ),
        in_specs=[ANY] * 10,
        out_specs=(VMEM, VMEM, ANY, ANY),
        scratch_shapes=[
            pltpu.VMEM(x.shape, BF16), pltpu.SMEM(lens.shape, jnp.int32), pltpu.VMEM(chosen_t.shape, jnp.int32),
            pltpu.VMEM(gain.shape, BF16), pltpu.VMEM(freq.shape, F32),
            pltpu.VMEM(wq.shape, BF16), pltpu.VMEM(wk.shape, BF16), pltpu.VMEM(wv.shape, BF16),
            pltpu.VMEM(k_cache.shape, BF16), pltpu.VMEM(v_cache.shape, BF16),
            pltpu.VMEM((rows, 256), F32), pltpu.VMEM((rows, 256), F32), pltpu.VMEM((rows, 256), F32),
            pltpu.VMEM((2 * rows, 128), F32),
            pltpu.SemaphoreType.DMA((8,)),
            pltpu.SemaphoreType.DMA((steps,)), pltpu.SemaphoreType.DMA((steps,)),
            pltpu.SemaphoreType.DMA((steps,)), pltpu.SemaphoreType.DMA((steps,)),
        ],
        compiler_params=pltpu.CompilerParams(vmem_limit_bytes=16 * 1024 * 1024),
    )(*in_hbm(x, lens, chosen_t, gain, freq, wq, wk, wv, k_cache, v_cache))


ORDER = (6, 2, 4, 7, 3, 5, 1)


def sum_kernel(n_ahead, project, *refs):
    if project:
        heads_ref, wo, *refs = refs
    else:
        part_ref, *refs = refs
    base_ref, *refs = refs
    ahead_hbm, (out_ref, *ahead), (inbox, piece, sems, *refs) = refs[:n_ahead], refs[n_ahead:2 * n_ahead + 1], refs[2 * n_ahead + 1:]
    me = lax.axis_index("tp")
    core, xx, yy = lax.rem(me, 2), lax.rem(me // 2, 2), me // 4
    cols = base_ref.shape[1] // 8

    def peer(m):
        return (1 - yy if m & 4 else yy) * 4 + (1 - xx if m & 2 else xx) * 2 + (1 - core if m & 1 else core)

    def columns(j):
        return pl.ds(pl.multiple_of(j * cols, cols), cols)

    def send(src, dst, m, phase):
        return pltpu.make_async_remote_copy(
            src_ref=src, dst_ref=dst, send_sem=sems.at[phase, m], recv_sem=sems.at[phase + 1, m],
            device_id={"tp": peer(m)}, device_id_type=pl.DeviceIdType.MESH)

    barrier = pltpu.get_barrier_semaphore()
    for m in ORDER:
        pl.semaphore_signal(barrier, inc=1, device_id={"tp": peer(m)}, device_id_type=pl.DeviceIdType.MESH)
    loads = []
    if project:
        part_ref, load_sems = refs
        loads = [pltpu.make_async_copy(src.at[pl.ds(e, 2)], dst.at[pl.ds(e, 2)], load_sems.at[m, e // 2])
                 for e in range(0, HELD, 2) for m, (src, dst) in enumerate(zip(ahead_hbm, ahead))]
        for load in loads:
            load.start()
        for j in range(0, base_ref.shape[1], cols):
            part_ref[:, j:j + cols] = jnp.dot(heads_ref[...], wo[:, j:j + cols], preferred_element_type=F32)
    pl.semaphore_wait(barrier, len(ORDER))

    first = {m: send(part_ref.at[:, columns(peer(m))], inbox.at[m - 1], m, 0) for m in ORDER}
    for m in ORDER:
        first[m].start()
    total = part_ref[:, columns(me)]
    for m in (1, 2, 4, 3, 5, 6, 7):
        first[m].wait_recv()
        total = total + inbox[m - 1]
    piece[...] = (base_ref[:, columns(me)].astype(F32) + total).astype(BF16)
    second = [send(piece, out_ref.at[:, columns(me)], m, 2) for m in ORDER]
    for copy in second:
        copy.start()
    out_ref[:, columns(me)] = piece[...]
    for m in ORDER:
        first[m].wait_send()
    for copy in second:
        copy.wait()
    for load in loads:
        load.wait()


def add_sum(partial, base, collective_id, ahead=()):
    rows, width = base.shape
    project = len(partial) == 2
    scratch = [pltpu.VMEM((7, rows, width // 8), F32), pltpu.VMEM((rows, width // 8), BF16), pltpu.SemaphoreType.DMA((4, 8))]
    if project:
        scratch += [pltpu.VMEM((rows, width), F32), pltpu.SemaphoreType.DMA((3, HELD // 2))]
    return pl.pallas_call(
        functools.partial(sum_kernel, len(ahead), project),
        name="add_sum",
        out_shape=[pltpu.VMEM(base.shape, BF16)] + [pltpu.VMEM((HELD, *a.shape[1:]), a.dtype) for a in ahead],
        in_specs=[VMEM] * (len(partial) + 1) + [ANY] * len(ahead),
        out_specs=[VMEM] * (1 + len(ahead)),
        scratch_shapes=scratch,
        compiler_params=pltpu.CompilerParams(collective_id=collective_id, has_side_effects=True, vmem_limit_bytes=4 * 1024 * 1024),
    )(*partial, base, *in_hbm(*ahead))


def experts_kernel(list_ref, x_ref, chosen_ref, gain_ref, wr_ref, held_g, held_u, held_d, gate_hbm, up_hbm, down_hbm, out_ref,
                   gates, h_ref, ring_g, ring_u, ring_d, sem):
    rows, width = x_ref.shape
    held, count = list_ref[0, 126], list_ref[0, 127]
    rest = count - held

    def fetch(i, go):
        slot = lax.rem(i, RING)
        e = list_ref[0, held + i]
        for m, (hbm, ring) in enumerate(((gate_hbm, ring_g), (up_hbm, ring_u), (down_hbm, ring_d))):
            copy = pltpu.make_async_copy(hbm.at[e], ring.at[slot], sem.at[m, slot])
            if go:
                copy.start()
            else:
                copy.wait()

    def fetch_pair(p, go):
        for i in (2 * p, 2 * p + 1):
            @pl.when(i < rest)
            def _():
                fetch(i, go)

    for p in range(RING // 2 - 1):
        fetch_pair(p, True)

    h = norm_rows(x_ref[...], gain_ref[...])
    h_ref[...] = h
    logits = lax.dot_general(wr_ref[...], h, NT, preferred_element_type=F32)
    experts = logits.shape[0]
    sub = lax.broadcasted_iota(jnp.int32, (experts, rows), 0)
    hit = chosen_ref[0:1, :] == sub
    for k in range(1, chosen_ref.shape[0]):
        hit = hit | (chosen_ref[k:k + 1, :] == sub)
    top = jnp.max(jnp.where(hit, logits, MASK_FILL), axis=0, keepdims=True)
    e = jnp.where(hit, jnp.exp(jnp.where(hit, logits - top, 0.0)), 0.0)
    gates[...] = (e / jnp.sum(e, axis=0, keepdims=True)).T
    out_ref[...] = jnp.zeros_like(out_ref)
    lane = lax.broadcasted_iota(jnp.int32, (rows, experts), 1)
    tile = 512

    def wide(e, gate, up, weight):
        g = u = None
        for t in range(0, width, tile):
            hk = h_ref[:, t:t + tile]
            gt = lax.dot_general(gate[:, t:t + tile], hk, NT, preferred_element_type=F32)
            ut = lax.dot_general(hk, up[:, t:t + tile], NT, preferred_element_type=F32)
            g, u = (gt, ut) if g is None else (g + gt, u + ut)
        column = weight * jnp.sum(jnp.where(lane == e, gates[...], 0.0), axis=1, keepdims=True)
        return (column * jax.nn.silu(g.T) * u).astype(BF16)

    def narrow(z, down):
        for t in range(0, width, tile):
            out_ref[:, t:t + tile] += jnp.dot(z, down[:, t:t + tile], preferred_element_type=F32)

    def block(items):
        zs = [wide(e, gate, up, weight) for e, gate, up, _, weight in items]
        for z, (_, _, _, down, _) in zip(zs, items):
            narrow(z, down)

    def held_item(j):
        e = list_ref[0, j]
        return e, held_g.at[e], held_u.at[e], held_d.at[e], 1.0

    def ring_item(i):
        at = jnp.minimum(i, rest - 1)
        slot = lax.rem(at, RING)
        weight = jnp.where(i < rest, 1.0, 0.0)
        return list_ref[0, held + at], ring_g.at[slot], ring_u.at[slot], ring_d.at[slot], weight

    def step(p, done):
        fetch_pair(p + RING // 2 - 1, True)
        fetch_pair(p, False)

        @pl.when(done < held)
        def _():
            block([ring_item(2 * p), ring_item(2 * p + 1), held_item(done)])

        @pl.when(done >= held)
        def _():
            block([ring_item(2 * p), ring_item(2 * p + 1)])

        return jnp.minimum(done + 1, held)

    def remaining(j, carry):
        block([held_item(j)])
        return carry

    done = lax.fori_loop(0, (rest + 1) // 2, step, 0)
    lax.fori_loop(done, held, remaining, 0)


def experts_part(ids, x1, chosen_t, gain, wr_t, held, gate_t, up_t, down):
    rows, width = x1.shape
    n_experts, hidden = gate_t.shape[:2]
    return pl.pallas_call(
        experts_kernel,
        name="experts",
        out_shape=pltpu.VMEM((rows, width), F32),
        in_specs=[SMEM, VMEM, VMEM, VMEM, VMEM, VMEM, VMEM, VMEM, ANY, ANY, ANY],
        out_specs=VMEM,
        scratch_shapes=[
            pltpu.VMEM((rows, n_experts), F32), pltpu.VMEM((rows, width), BF16),
            pltpu.VMEM((RING, hidden, width), BF16), pltpu.VMEM((RING, hidden, width), BF16), pltpu.VMEM((RING, hidden, width), BF16),
            pltpu.SemaphoreType.DMA((3, RING)),
        ],
        compiler_params=pltpu.CompilerParams(vmem_limit_bytes=15 * 1024 * 1024),
    )(ids, x1, chosen_t, gain, wr_t, *held, *in_hbm(gate_t, up_t, down))


def solution(mesh):
    cache_spec = P("dp", None, "tp", None)
    in_specs = (P("dp", None), cache_spec, cache_spec, P("dp"), P("dp", None), P(None), P(None, "tp"), P(None, "tp"), P(None, "tp"), P("tp", None), P(None), P(None, None), P(None, None, "tp"), P(None, None, "tp"), P(None, "tp", None))
    out_specs = (P("dp", None), cache_spec, cache_spec)
    freq = (np.float32(ROPE_THETA) ** (-np.arange(0, 128, 2, dtype=np.float32) / np.float32(128))).astype(np.float32)
    freq = np.concatenate([freq, freq])[None, :]

    def layer_shard(hidden_in, k_cache, v_cache, seq_lens, chosen, g_attn, w_q, w_k, w_v, w_o, g_moe, w_router, w_gate, w_up, w_down):
        rows, slots, kv_heads, dim = k_cache.shape
        width = hidden_in.shape[1]
        chosen_t = chosen.T
        flat = (rows, slots * kv_heads, dim)
        heads, ids, k_next, v_next = attention(
            hidden_in, seq_lens, chosen_t, g_attn.reshape(width // 128, 128), jnp.asarray(freq), w_q, w_k, w_v,
            k_cache.reshape(flat), v_cache.reshape(flat))
        experts = (jnp.swapaxes(w_gate, 1, 2), jnp.swapaxes(w_up, 1, 2), w_down)
        x1, *held = add_sum((heads, w_o), hidden_in, 1, experts)
        moe = experts_part(ids, x1, chosen_t, g_moe.reshape(width // 128, 128), w_router.T, held, *experts)
        out, = add_sum((moe,), x1, 2)
        return out, k_next.reshape(k_cache.shape), v_next.reshape(v_cache.shape)

    return jax.shard_map(layer_shard, mesh=mesh, in_specs=in_specs, out_specs=out_specs, check_vma=False)
```
